8 devices in a mesh: data: 1 (over z), expert: 8 (over y, x, core).
Axes of the slice: x: 2, y: 2, z: 1, core: 2. Of those that a mesh axis runs over, the one named last changes fastest.
Arguments:
- x_tokens: bfloat16 [512, 1536], P(('data', 'expert'))
- y_mid: bfloat16 [512, 1536], P(('data', 'expert'))
- dy_out: bfloat16 [512, 1536], P(('data', 'expert'))
- experts_one: int32 [512, 8], P(('data', 'expert'))
- gates_one: float32 [512, 8], P(('data', 'expert'))
- slots_one: int32 [512, 8], P(('data', 'expert'))
- experts_two: int32 [512, 8], P(('data', 'expert'))
- gates_two: float32 [512, 8], P(('data', 'expert'))
- slots_two: int32 [512, 8], P(('data', 'expert'))
- w_gate_one: bfloat16 [40, 1536, 512], P('expert')
- w_up_one: bfloat16 [40, 1536, 512], P('expert')
- w_down_one: bfloat16 [40, 512, 1536], P('expert')
- w_gate_two: bfloat16 [40, 1536, 512], P('expert')
- w_up_two: bfloat16 [40, 1536, 512], P('expert')
- w_down_two: bfloat16 [40, 512, 1536], P('expert')
Outputs:
- output 1: bfloat16 [512, 1536], P(('data', 'expert'))
- output 2: float32 [40, 1536, 512], P(('data', 'expert'))
- output 3: float32 [40, 1536, 512], P(('data', 'expert'))
- output 4: float32 [40, 512, 1536], P(('data', 'expert'))
- output 5: float32 [40, 1536, 512], P(('data', 'expert'))
- output 6: float32 [40, 1536, 512], P(('data', 'expert'))
- output 7: float32 [40, 512, 1536], P(('data', 'expert'))
All inputs are finite; a program needn't handle non-finite values.
Results may differ from the reference program's by a relative error of at most 0.0132769.
Values are sent between devices in bfloat16 or wider.
A program may use at most 1 GiB of HBM per device.

```python
import jax
import jax.numpy as jnp
from jax import lax

MODEL_DIM = 1536
FFN_DIM = 512
EXPERTS = 40
TOP_K = 8
TOKENS_DEV = 64
GROUP_SIZE = 8

TOKENS_PART = GROUP_SIZE * TOKENS_DEV
CAPACITY = 8 * ((3 * TOP_K * TOKENS_DEV + 16 * EXPERTS - 1) // (16 * EXPERTS))
TOTAL_ROWS = GROUP_SIZE * EXPERTS * CAPACITY


def draw_routing(key):
    key_noise, key_bias, key_hot = jax.random.split(key, 3)
    noise_int = jax.random.randint(key_noise, (TOKENS_PART, EXPERTS), 0, 4096)
    expert_bias = jax.random.randint(key_bias, (EXPERTS,), 0, 512)
    hot_expert = jax.random.randint(key_hot, (), 0, EXPERTS)
    expert_ids = jnp.arange(EXPERTS, dtype=jnp.int32)
    local_tok = jnp.arange(TOKENS_PART, dtype=jnp.int32) % TOKENS_DEV
    boost_int = jnp.where((local_tok[:, None] < CAPACITY) & (expert_ids[None, :] == hot_expert), 8192, 0)
    score_int = (noise_int + expert_bias[None, :] + boost_int) * EXPERTS + expert_ids[None, :]
    top_vals, experts = lax.top_k(score_int, TOP_K)
    flat_ids = experts.reshape(GROUP_SIZE, TOKENS_DEV * TOP_K)
    onehot = (flat_ids[:, :, None] == expert_ids[None, None, :]).astype(jnp.int32)
    slot_rank = jnp.sum((jnp.cumsum(onehot, axis=1) - 1) * onehot, axis=2)
    slots = jnp.where(slot_rank < CAPACITY, slot_rank, -1).reshape(TOKENS_PART, TOP_K)
    return experts.astype(jnp.int32), slots.astype(jnp.int32)


def draw_weight(key, shape, fan_in):
    return (jax.random.normal(key, shape, jnp.float32) * fan_in ** -0.5).astype(jnp.bfloat16)


def setup_inputs(seed: int = 0, part: int = 0) -> dict:
    key_part = jax.random.fold_in(jax.random.key(seed), part)
    keys = jax.random.split(key_part, 7)
    shared = jax.random.split(jax.random.key(seed + 1), 6)
    tok_shape = (TOKENS_PART, MODEL_DIM)
    route_shape = (TOKENS_PART, TOP_K)
    up_shape = (EXPERTS, MODEL_DIM, FFN_DIM)
    down_shape = (EXPERTS, FFN_DIM, MODEL_DIM)
    gate_scale = TOP_K ** -0.5
    experts_one, slots_one = draw_routing(keys[3])
    experts_two, slots_two = draw_routing(keys[4])
    return {
        "x_tokens": jax.random.normal(keys[0], tok_shape, jnp.float32).astype(jnp.bfloat16),
        "y_mid": jax.random.normal(keys[1], tok_shape, jnp.float32).astype(jnp.bfloat16),
        "dy_out": jax.random.normal(keys[2], tok_shape, jnp.float32).astype(jnp.bfloat16),
        "experts_one": experts_one,
        "gates_one": jax.random.uniform(keys[5], route_shape, jnp.float32, 0.5, 1.5) * gate_scale,
        "slots_one": slots_one,
        "experts_two": experts_two,
        "gates_two": jax.random.uniform(keys[6], route_shape, jnp.float32, 0.5, 1.5) * gate_scale,
        "slots_two": slots_two,
        "w_gate_one": draw_weight(shared[0], up_shape, MODEL_DIM),
        "w_up_one": draw_weight(shared[1], up_shape, MODEL_DIM),
        "w_down_one": draw_weight(shared[2], down_shape, FFN_DIM),
        "w_gate_two": draw_weight(shared[3], up_shape, MODEL_DIM),
        "w_up_two": draw_weight(shared[4], up_shape, MODEL_DIM),
        "w_down_two": draw_weight(shared[5], down_shape, FFN_DIM),
    }


def expert_grads(operands):
    x_rows, z_rows, w_gate, w_up, w_down = operands
    gate_act = jnp.dot(x_rows, w_gate, preferred_element_type=jnp.float32).astype(jnp.bfloat16).astype(jnp.float32)
    up_act = jnp.dot(x_rows, w_up, preferred_element_type=jnp.float32).astype(jnp.bfloat16).astype(jnp.float32)
    sig_gate = jax.nn.sigmoid(gate_act)
    silu_gate = gate_act * sig_gate
    hidden = (silu_gate * up_act).astype(jnp.bfloat16)
    d_hidden = jnp.dot(z_rows, w_down.T, preferred_element_type=jnp.float32)
    dw_down = jnp.dot(hidden.T, z_rows, preferred_element_type=jnp.float32)
    d_gate = (d_hidden * up_act * sig_gate * (1.0 + gate_act * (1.0 - sig_gate))).astype(jnp.bfloat16)
    d_up = (d_hidden * silu_gate).astype(jnp.bfloat16)
    dx_rows = (jnp.dot(d_gate, w_gate.T, preferred_element_type=jnp.float32) + jnp.dot(d_up, w_up.T, preferred_element_type=jnp.float32)).astype(jnp.bfloat16)
    dw_gate = jnp.dot(x_rows.T, d_gate, preferred_element_type=jnp.float32)
    dw_up = jnp.dot(x_rows.T, d_up, preferred_element_type=jnp.float32)
    return dx_rows, dw_gate, dw_up, dw_down


def layer_backward(inputs, cotangent, experts, gates, slots, w_gate, w_up, w_down):
    source = jnp.arange(TOKENS_PART, dtype=jnp.int32) // TOKENS_DEV
    target = jnp.where(slots >= 0, (source[:, None] * EXPERTS + experts) * CAPACITY + slots, TOTAL_ROWS).reshape(-1)
    x_copies = jnp.repeat(inputs, TOP_K, axis=0)
    z_copies = (gates[:, :, None] * cotangent[:, None, :].astype(jnp.float32)).astype(jnp.bfloat16).reshape(TOKENS_PART * TOP_K, MODEL_DIM)
    x_buffer = jnp.zeros((TOTAL_ROWS + 1, MODEL_DIM), jnp.bfloat16).at[target].add(x_copies)
    z_buffer = jnp.zeros((TOTAL_ROWS + 1, MODEL_DIM), jnp.bfloat16).at[target].add(z_copies)
    by_source = (GROUP_SIZE, EXPERTS, CAPACITY, MODEL_DIM)
    by_expert = (EXPERTS, GROUP_SIZE * CAPACITY, MODEL_DIM)
    x_rows = x_buffer[:TOTAL_ROWS].reshape(by_source).transpose(1, 0, 2, 3).reshape(by_expert)
    z_rows = z_buffer[:TOTAL_ROWS].reshape(by_source).transpose(1, 0, 2, 3).reshape(by_expert)
    dx_rows, dw_gate, dw_up, dw_down = lax.map(expert_grads, (x_rows, z_rows, w_gate, w_up, w_down))
    returned = dx_rows.reshape(EXPERTS, GROUP_SIZE, CAPACITY, MODEL_DIM).transpose(1, 0, 2, 3).reshape(TOTAL_ROWS, MODEL_DIM)
    returned = jnp.concatenate([returned, jnp.zeros((1, MODEL_DIM), jnp.bfloat16)], axis=0)
    per_copy = returned[target].reshape(TOKENS_PART, TOP_K, MODEL_DIM).astype(jnp.float32)
    return jnp.sum(per_copy, axis=1), dw_gate, dw_up, dw_down


def reference(x_tokens, y_mid, dy_out, experts_one, gates_one, slots_one, experts_two, gates_two, slots_two, w_gate_one, w_up_one, w_down_one, w_gate_two, w_up_two, w_down_two):
    grads_two = layer_backward(y_mid, dy_out, experts_two, gates_two, slots_two, w_gate_two, w_up_two, w_down_two)
    dy_mid = (dy_out.astype(jnp.float32) + grads_two[0]).astype(jnp.bfloat16)
    grads_one = layer_backward(x_tokens, dy_mid, experts_one, gates_one, slots_one, w_gate_one, w_up_one, w_down_one)
    dx_tokens = (dy_mid.astype(jnp.float32) + grads_one[0]).astype(jnp.bfloat16)
    return (dx_tokens, grads_one[1], grads_one[2], grads_one[3], grads_two[1], grads_two[2], grads_two[3])
```

```python
import functools
import jax
import jax.numpy as jnp
from jax import lax
from jax.experimental import pallas as pl
from jax.experimental.pallas import tpu as pltpu
from jax.sharding import PartitionSpec as P

MESH = pl.DeviceIdType.MESH
F32 = jnp.float32
BF16 = jnp.bfloat16
CAP = 24
LOCAL = 5
D = 1536
F = 512
TOK = 64
HALF_ROWS = 4 * CAP
ROWS = 8 * CAP
STEP = 512


def place():
    me = lax.axis_index("expert")
    core, x, y = me % 2, (me // 2) % 2, me // 4
    ident = lambda xx, yy, cc: 4 * yy + 2 * xx + cc
    ids = {
        "me": me,
        "partner": ident(x, y, 1 - core),
        "x": ident(1 - x, y, core),
        "y": ident(x, 1 - y, core),
        "diag": ident(1 - x, 1 - y, core),
        "prim": ident(x + (1 - core) * (1 - 2 * x), y + core * (1 - 2 * y), core),
        "sec": ident(x + core * (1 - 2 * x), y + (1 - core) * (1 - 2 * y), core),
        "p_prim": ident(x + core * (1 - 2 * x), y + (1 - core) * (1 - 2 * y), 1 - core),
        "p_sec": ident(x + (1 - core) * (1 - 2 * x), y + core * (1 - 2 * y), 1 - core),
        "p_diag": ident(1 - x, 1 - y, 1 - core),
    }
    return ids, core, x, y


def barrier(ids):
    sem = pltpu.get_barrier_semaphore()
    for peer in ("partner", "x", "y"):
        pl.semaphore_signal(sem, inc=1, device_id={"expert": ids[peer]}, device_id_type=MESH)
    pl.semaphore_wait(sem, 3)


def block(ref, ident):
    return ref.at[pl.ds(pl.multiple_of(ident * TOK, TOK), TOK)]


class Gather:
    ROUTES = (("me", "partner"), ("me", "prim"), ("me", "sec"), ("prim", "sec"), ("prim", "partner"), ("sec", "partner"), ("diag", "partner"))
    ARRIVE = ("partner", "prim", "sec", "diag", "p_prim", "p_sec", "p_diag")

    def __init__(self, ids, ref, send, recv):
        self.ids, self.ref, self.send, self.recv = ids, ref, send, recv

    def copy(self, k):
        what, where = self.ROUTES[k]
        part = block(self.ref, self.ids[what])
        return pltpu.make_async_remote_copy(src_ref=part, dst_ref=part, send_sem=self.send.at[k], recv_sem=self.recv.at[k], device_id={"expert": self.ids[where]}, device_id_type=MESH)

    def arrived(self, k):
        part = block(self.ref, self.ids[self.ARRIVE[k]])
        pltpu.make_async_remote_copy(src_ref=part, dst_ref=part, send_sem=self.send.at[k], recv_sem=self.recv.at[k], device_id={"expert": self.ids["partner"]}, device_id_type=MESH).wait_recv()

    def start(self):
        for k in (1, 2, 0):
            self.copy(k).start()

    def relay_prim(self):
        self.arrived(1)
        self.copy(3).start()
        self.copy(4).start()

    def relay_rest(self):
        self.arrived(2)
        self.copy(5).start()
        self.arrived(3)
        self.copy(6).start()

    def finish(self):
        for k in (0, 4, 5, 6):
            self.arrived(k)

    def drain(self):
        for k in range(7):
            self.copy(k).wait_send()


def build_onehot(table, base, me, onehot, gate_col):
    for h in range(2):
        cols = slice(h * 256, (h + 1) * 256)
        keys = [table[base + j : base + j + 1, cols] for j in range(8)]
        gates = [table[base + 8 + j : base + 9 + j, cols] for j in range(8)]
        for e in range(LOCAL):
            row = (lax.broadcasted_iota(jnp.int32, (HALF_ROWS, 256), 0) + (e + me * LOCAL) * HALF_ROWS).astype(F32)
            gate = jnp.zeros((HALF_ROWS, 256), F32)
            hit = jnp.zeros((HALF_ROWS, 256), F32)
            for j in range(8):
                match = row == keys[j]
                gate = jnp.where(match, gates[j], gate)
                hit = jnp.where(match, 1.0, hit)
            onehot[h, e * HALF_ROWS : (e + 1) * HALF_ROWS, :] = hit.astype(BF16)
            gate_col[h, e * HALF_ROWS : (e + 1) * HALF_ROWS, :] = jnp.broadcast_to(jnp.sum(gate, axis=1, keepdims=True), (HALF_ROWS, 128))


def take_rows(onehot, tokens, rows, gate_col=None):
    for h in range(2):
        for n in range(D // STEP):
            cols = slice(n * STEP, (n + 1) * STEP)
            out = jnp.dot(onehot[h], tokens[h * 256 : (h + 1) * 256, cols], preferred_element_type=F32)
            if gate_col is not None:
                out = out * gate_col[h, :, 0:1]
            out = out.astype(BF16)
            for e in range(LOCAL):
                rows[e, h * HALF_ROWS : (h + 1) * HALF_ROWS, cols] = out[e * HALF_ROWS : (e + 1) * HALF_ROWS]


def forward_expert(e, u, w1, w3, a, b, hid):
    act = jnp.dot(u[e], w1[e], preferred_element_type=F32).astype(BF16)
    up = jnp.dot(u[e], w3[e], preferred_element_type=F32).astype(BF16)
    a[e] = act
    b[e] = up
    wide = act.astype(F32)
    hid[e] = (wide * jax.nn.sigmoid(wide) * up.astype(F32)).astype(BF16)


TRANS_B = (((1,), (1,)), ((), ()))
TRANS_A = (((0,), (0,)), ((), ()))


def backward_expert(e, z, w1, w3, w2, a, b, dxr):
    dh = lax.dot_general(z[e], w2[e], TRANS_B, preferred_element_type=F32)
    act = a[e].astype(F32)
    up = b[e].astype(F32)
    sig = jax.nn.sigmoid(act)
    da = (dh * up * sig * (1.0 + act * (1.0 - sig))).astype(BF16)
    db = (dh * (act * sig)).astype(BF16)
    a[e] = da
    b[e] = db
    for n in range(D // STEP):
        cols = slice(n * STEP, (n + 1) * STEP)
        dx = lax.dot_general(da, w1[e, cols, :], TRANS_B, preferred_element_type=F32) + lax.dot_general(db, w3[e, cols, :], TRANS_B, preferred_element_type=F32)
        dx = dx.astype(BF16)
        for h in range(2):
            dxr[h, pl.ds(pl.multiple_of(e * HALF_ROWS, HALF_ROWS), HALF_ROWS), cols] = dx[h * HALF_ROWS : (h + 1) * HALF_ROWS]


def return_sums(ids, core, x, y, onehot, dxr, sums, inbox, send, recv, outs):
    def exchange(yy, xx):
        theirs = 4 * yy + 2 * xx + (1 - core)
        return pltpu.make_async_remote_copy(src_ref=block(sums, theirs), dst_ref=inbox.at[2 * yy + xx], send_sem=send.at[2 * yy + xx], recv_sem=recv.at[2 * yy + xx], device_id={"expert": ids["partner"]}, device_id_type=MESH)

    for h in range(2):
        for n in range(D // STEP):
            cols = slice(n * STEP, (n + 1) * STEP)
            sums[h * 256 : (h + 1) * 256, cols] = lax.dot_general(onehot[h], dxr[h, :, cols], TRANS_A, preferred_element_type=F32)
        for xx in range(2):
            exchange(h, xx).start()
    for h in range(2):
        for xx in range(2):
            exchange(h, xx).wait_recv()
    for name, xx, yy, out in (("me", x, y, outs[0]), ("x", 1 - x, y, outs[1]), ("y", x, 1 - y, outs[2]), ("diag", 1 - x, 1 - y, outs[3])):
        out[...] = block(sums, ids[name])[...] + inbox[2 * yy + xx]
    for h in range(2):
        for xx in range(2):
            exchange(h, xx).wait_send()


def fetch_weights(hbm, vmem, sems):
    copies = []
    for e in range(LOCAL):
        for k in range(3):
            copies.append(pltpu.make_async_copy(hbm[k].at[e], vmem[k].at[e], sems.at[k, e]))
    return copies


def layer_two_kernel(tab_h, y_h, dy_h, x_h, w1_h, w3_h, w2_h,
                     u_o, z_o, hid_o, da_o, db_o, xall_o, table_o, s_me, s_x, s_y, s_d,
                     tab, yall, dall, xall, w1, w3, w2, onehot, gate_col, u, z, a, b, hid, dxr, sums, inbox,
                     lsem, wsem, osem, gsend, grecv, xsend, xrecv):
    ids, core, x, y = place()
    local = [pltpu.make_async_copy(src, block(dst, ids["me"]), lsem.at[i]) for i, (src, dst) in enumerate(((tab_h, tab), (y_h, yall), (dy_h, dall), (x_h, xall)))]
    for c in local:
        c.start()
    weights = fetch_weights((w1_h, w3_h, w2_h), (w1, w3, w2), wsem)
    for c in weights:
        c.start()
    barrier(ids)
    gt, gy, gd, gx = [Gather(ids, ref, gsend.at[i], grecv.at[i]) for i, ref in enumerate((tab, yall, dall, xall))]
    for c, g in zip(local[:3], (gt, gy, gd)):
        c.wait()
    gt.start()
    gy.start()
    gt.relay_prim()
    gt.relay_rest()
    gt.finish()
    table_o[...] = jnp.transpose(tab[...])[0:32, :]
    build_onehot(table_o, 0, ids["me"], onehot, gate_col)
    gy.relay_prim()
    gd.start()
    gy.relay_rest()
    gy.finish()
    take_rows(onehot, yall, u)
    for e in range(LOCAL):
        weights[3 * e].wait()
        weights[3 * e + 1].wait()
    store_u = pltpu.make_async_copy(u, u_o, osem.at[0])
    store_u.start()
    forward = lambda e, carry: (forward_expert(e, u, w1, w3, a, b, hid), carry)[1]
    lax.fori_loop(0, 1, forward, 0)
    gd.relay_prim()
    local[3].wait()
    gx.start()
    lax.fori_loop(1, LOCAL, forward, 0)
    gd.relay_rest()
    gd.finish()
    take_rows(onehot, dall, z, gate_col)
    gx.relay_prim()
    for e in range(LOCAL):
        weights[3 * e + 2].wait()
    store_z = pltpu.make_async_copy(z, z_o, osem.at[1])
    store_h = pltpu.make_async_copy(hid, hid_o, osem.at[2])
    store_z.start()
    store_h.start()
    lax.fori_loop(0, LOCAL, lambda e, carry: (backward_expert(e, z, w1, w3, w2, a, b, dxr), carry)[1], 0)
    gx.relay_rest()
    store_a = pltpu.make_async_copy(a, da_o, osem.at[3])
    store_b = pltpu.make_async_copy(b, db_o, osem.at[4])
    store_a.start()
    store_b.start()
    gx.finish()
    store_x = pltpu.make_async_copy(xall, xall_o, osem.at[5])
    store_x.start()
    return_sums(ids, core, x, y, onehot, dxr, sums, inbox, xsend, xrecv, (s_me, s_x, s_y, s_d))
    for g in (gt, gy, gd, gx):
        g.drain()
    for c in (store_u, store_z, store_h, store_a, store_b, store_x):
        c.wait()


def layer_one_kernel(dy_h, r_me, r_x, r_y, r_d, table, xall_h, w1_h, w3_h, w2_h,
                     u_o, z_o, hid_o, da_o, db_o, dy1_o, s_me, s_x, s_y, s_d,
                     dall, xall, w1, w3, w2, onehot, gate_col, u, z, a, b, hid, dxr, sums, inbox,
                     lsem, wsem, osem, gsend, grecv, xsend, xrecv):
    ids, core, x, y = place()
    load_x = pltpu.make_async_copy(xall_h, xall, lsem.at[0])
    load_x.start()
    weights = fetch_weights((w1_h, w3_h, w2_h), (w1, w3, w2), wsem)
    for c in weights:
        c.start()
    dy1 = (dy_h[...].astype(F32) + ((r_me[...] + r_x[...]) + (r_y[...] + r_d[...]))).astype(BF16)
    dall[pl.ds(pl.multiple_of(ids["me"] * TOK, TOK), TOK), :] = dy1
    dy1_o[...] = dy1
    barrier(ids)
    gd = Gather(ids, dall, gsend, grecv)
    gd.start()
    build_onehot(table, 16, ids["me"], onehot, gate_col)
    load_x.wait()
    take_rows(onehot, xall, u)
    store_u = pltpu.make_async_copy(u, u_o, osem.at[0])
    store_u.start()
    for e in range(LOCAL):
        weights[3 * e].wait()
        weights[3 * e + 1].wait()
    forward = lambda e, carry: (forward_expert(e, u, w1, w3, a, b, hid), carry)[1]
    lax.fori_loop(0, 2, forward, 0)
    gd.relay_prim()
    lax.fori_loop(2, LOCAL, forward, 0)
    gd.relay_rest()
    gd.finish()
    take_rows(onehot, dall, z, gate_col)
    for e in range(LOCAL):
        weights[3 * e + 2].wait()
    store_z = pltpu.make_async_copy(z, z_o, osem.at[1])
    store_h = pltpu.make_async_copy(hid, hid_o, osem.at[2])
    store_z.start()
    store_h.start()
    lax.fori_loop(0, LOCAL, lambda e, carry: (backward_expert(e, z, w1, w3, w2, a, b, dxr), carry)[1], 0)
    store_a = pltpu.make_async_copy(a, da_o, osem.at[3])
    store_b = pltpu.make_async_copy(b, db_o, osem.at[4])
    store_a.start()
    store_b.start()
    return_sums(ids, core, x, y, onehot, dxr, sums, inbox, xsend, xrecv, (s_me, s_x, s_y, s_d))
    gd.drain()
    for c in (store_u, store_z, store_h, store_a, store_b):
        c.wait()


HBM_SPEC = pl.BlockSpec(memory_space=pl.ANY)
VMEM_SPEC = pl.BlockSpec(memory_space=pltpu.VMEM)


def compute_scratch():
    return [
        pltpu.VMEM((LOCAL, D, F), BF16), pltpu.VMEM((LOCAL, D, F), BF16), pltpu.VMEM((LOCAL, F, D), BF16),
        pltpu.VMEM((2, LOCAL * HALF_ROWS, 256), BF16), pltpu.VMEM((2, LOCAL * HALF_ROWS, 128), F32),
        pltpu.VMEM((LOCAL, ROWS, D), BF16), pltpu.VMEM((LOCAL, ROWS, D), BF16),
        pltpu.VMEM((LOCAL, ROWS, F), BF16), pltpu.VMEM((LOCAL, ROWS, F), BF16), pltpu.VMEM((LOCAL, ROWS, F), BF16),
        pltpu.VMEM((2, LOCAL * HALF_ROWS, D), BF16), pltpu.VMEM((8 * TOK, D), F32), pltpu.VMEM((4, TOK, D), F32),
    ]


ROW_OUTS = [jax.ShapeDtypeStruct((LOCAL, ROWS, D), BF16)] * 2 + [jax.ShapeDtypeStruct((LOCAL, ROWS, F), BF16)] * 3
SUM_OUTS = [jax.ShapeDtypeStruct((TOK, D), F32)] * 4
DMA = pltpu.SemaphoreType.DMA


def layer_two(tab, y_mid, dy_out, x_tokens, w1, w3, w2):
    all_tok = pltpu.VMEM((8 * TOK, D), BF16)
    return pl.pallas_call(
        layer_two_kernel, name="layer_two",
        out_shape=ROW_OUTS + [jax.ShapeDtypeStruct((8 * TOK, D), BF16), jax.ShapeDtypeStruct((32, 8 * TOK), F32)] + SUM_OUTS,
        in_specs=[HBM_SPEC] * 7, out_specs=[HBM_SPEC] * 6 + [VMEM_SPEC] * 5,
        scratch_shapes=[pltpu.VMEM((8 * TOK, 128), F32), all_tok, all_tok, all_tok] + compute_scratch()
        + [DMA((4,)), DMA((3, LOCAL)), DMA((6,)), DMA((4, 7)), DMA((4, 7)), DMA((4,)), DMA((4,))],
        compiler_params=pltpu.CompilerParams(collective_id=0, has_side_effects=True, vmem_limit_bytes=60 * 2**20),
        cost_estimate=pl.CostEstimate(flops=16 * 10**9, bytes_accessed=36 * 2**20, transcendentals=0),
    )(tab, y_mid, dy_out, x_tokens, w1, w3, w2)


def layer_one(dy_out, returned, table, xall, w1, w3, w2):
    all_tok = pltpu.VMEM((8 * TOK, D), BF16)
    return pl.pallas_call(
        layer_one_kernel, name="layer_one",
        out_shape=ROW_OUTS + [jax.ShapeDtypeStruct((TOK, D), BF16)] + SUM_OUTS,
        in_specs=[VMEM_SPEC] * 6 + [HBM_SPEC] * 4, out_specs=[HBM_SPEC] * 5 + [VMEM_SPEC] * 5,
        scratch_shapes=[all_tok, all_tok] + compute_scratch()
        + [DMA((1,)), DMA((3, LOCAL)), DMA((5,)), DMA((7,)), DMA((7,)), DMA((4,)), DMA((4,))],
        compiler_params=pltpu.CompilerParams(collective_id=1, has_side_effects=True, vmem_limit_bytes=60 * 2**20),
        cost_estimate=pl.CostEstimate(flops=16 * 10**9, bytes_accessed=36 * 2**20, transcendentals=0),
    )(dy_out, *returned, table, xall, w1, w3, w2)


PARTS = 4


def weight_grad_kernel(u, da, db, hid, z, dw1, dw3, dw2):
    dw1[0] = lax.dot_general(u[0], da[0], TRANS_A, preferred_element_type=F32)
    dw3[0] = lax.dot_general(u[0], db[0], TRANS_A, preferred_element_type=F32)
    dw2[0] = lax.dot_general(hid[0], z[0], TRANS_A, preferred_element_type=F32)


def weight_grads(u, z, hid, da, db):
    whole = lambda cols: pl.BlockSpec((1, ROWS, cols), lambda e, p: (e, 0, 0))
    piece = lambda cols: pl.BlockSpec((1, ROWS, cols // PARTS), lambda e, p: (e, 0, p))
    out_rows = lambda rows, cols: pl.BlockSpec((1, rows // PARTS, cols), lambda e, p: (e, p, 0))
    return pl.pallas_call(
        weight_grad_kernel, name="weight_grads", grid=(LOCAL, PARTS),
        in_specs=[piece(D), whole(F), whole(F), piece(F), whole(D)],
        out_specs=[out_rows(D, F), out_rows(D, F), out_rows(F, D)],
        out_shape=[jax.ShapeDtypeStruct((LOCAL, D, F), F32)] * 2 + [jax.ShapeDtypeStruct((LOCAL, F, D), F32)],
        compiler_params=pltpu.CompilerParams(vmem_limit_bytes=32 * 2**20),
        cost_estimate=pl.CostEstimate(flops=18 * 10**9, bytes_accessed=56 * 2**20, transcendentals=0),
    )(u, da, db, hid, z)


def exchange_sums(sums):
    swap = lambda mask: [(i, i ^ mask) for i in range(8)]
    return (sums[0],) + tuple(lax.ppermute(sums[k], "expert", swap(mask)) for k, mask in ((1, 2), (2, 4), (3, 6)))


def routing_keys(experts, slots, gates):
    source = lax.axis_index("expert") % 4
    keys = jnp.where(slots >= 0, experts * HALF_ROWS + source * CAP + slots, -1)
    return [keys.astype(F32), gates]


def solution(mesh):
    tok_spec = P(("data", "expert"), None)
    weight_spec = P("expert", None, None)
    grad_spec = P(("data", "expert"), None, None)

    def local_step(x_tokens, y_mid, dy_out, experts_one, gates_one, slots_one, experts_two, gates_two, slots_two, w_gate_one, w_up_one, w_down_one, w_gate_two, w_up_two, w_down_two):
        parts = routing_keys(experts_two, slots_two, gates_two) + routing_keys(experts_one, slots_one, gates_one)
        tab = jnp.concatenate(parts + [jnp.zeros((TOK, 96), F32)], axis=1)
        *rows_two, xall, table, s0, s1, s2, s3 = layer_two(tab, y_mid, dy_out, x_tokens, w_gate_two, w_up_two, w_down_two)
        returned = exchange_sums((s0, s1, s2, s3))
        grads_two = weight_grads(*rows_two)
        *rows_one, dy_mid, s0, s1, s2, s3 = layer_one(dy_out, returned, table, xall, w_gate_one, w_up_one, w_down_one)
        r = exchange_sums((s0, s1, s2, s3))
        grads_one = weight_grads(*rows_one)
        dx_tokens = (dy_mid.astype(F32) + ((r[0] + r[1]) + (r[2] + r[3]))).astype(BF16)
        return (dx_tokens, *grads_one, *grads_two)

    return jax.shard_map(local_step, mesh=mesh, in_specs=(tok_spec,) * 9 + (weight_spec,) * 6, out_specs=(tok_spec,) + (grad_spec,) * 6, check_vma=False)
```

```python
import functools
import jax
import jax.numpy as jnp
from jax import lax
from jax.experimental import pallas as pl
from jax.experimental.pallas import tpu as pltpu
from jax.sharding import PartitionSpec as P

MESH = pl.DeviceIdType.MESH
F32 = jnp.float32
BF16 = jnp.bfloat16
CAP = 24
LOCAL = 5
D = 1536
F = 512
TOK = 64
HALF_ROWS = 4 * CAP
ROWS = 8 * CAP
STEP = 512


def place():
    me = lax.axis_index("expert")
    core, x, y = me % 2, (me // 2) % 2, me // 4
    ident = lambda xx, yy, cc: 4 * yy + 2 * xx + cc
    ids = {
        "me": me,
        "partner": ident(x, y, 1 - core),
        "x": ident(1 - x, y, core),
        "y": ident(x, 1 - y, core),
        "diag": ident(1 - x, 1 - y, core),
        "prim": ident(x + (1 - core) * (1 - 2 * x), y + core * (1 - 2 * y), core),
        "sec": ident(x + core * (1 - 2 * x), y + (1 - core) * (1 - 2 * y), core),
        "p_prim": ident(x + core * (1 - 2 * x), y + (1 - core) * (1 - 2 * y), 1 - core),
        "p_sec": ident(x + (1 - core) * (1 - 2 * x), y + core * (1 - 2 * y), 1 - core),
        "p_diag": ident(1 - x, 1 - y, 1 - core),
    }
    return ids, core, x, y


def barrier(ids):
    sem = pltpu.get_barrier_semaphore()
    for peer in ("partner", "x", "y"):
        pl.semaphore_signal(sem, inc=1, device_id={"expert": ids[peer]}, device_id_type=MESH)
    pl.semaphore_wait(sem, 3)


def block(ref, ident):
    return ref.at[pl.ds(pl.multiple_of(ident * TOK, TOK), TOK)]


class Gather:
    ROUTES = (("me", "partner"), ("me", "prim"), ("me", "sec"), ("prim", "sec"), ("prim", "partner"), ("sec", "partner"), ("diag", "partner"))
    ARRIVE = ("partner", "prim", "sec", "diag", "p_prim", "p_sec", "p_diag")

    def __init__(self, ids, ref, send, recv, pieces):
        self.ids, self.ref, self.send, self.recv, self.pieces = ids, ref, send, recv, pieces

    def part(self, ident, i):
        if self.pieces == 0:
            return self.ref.at[ident]
        size = TOK // self.pieces
        return self.ref.at[pl.ds(pl.multiple_of(ident * TOK + i * size, size), size)]

    def copy(self, k, i, what=None, where=None):
        what, where = what or self.ROUTES[k][0], where or self.ROUTES[k][1]
        part = self.part(self.ids[what], i)
        return pltpu.make_async_remote_copy(src_ref=part, dst_ref=part, send_sem=self.send.at[i, k], recv_sem=self.recv.at[i, k], device_id={"expert": self.ids[where]}, device_id_type=MESH)

    def arrived(self, k, i):
        self.copy(k, i, self.ARRIVE[k], "partner").wait_recv()

    def every(self):
        return range(max(self.pieces, 1))

    def start(self, k):
        for i in self.every():
            self.copy(k, i).start()

    def relay_prim(self, i):
        self.arrived(1, i)
        self.copy(3, i).start()
        self.copy(4, i).start()

    def relay_rest(self, i):
        self.arrived(2, i)
        self.copy(5, i).start()
        self.arrived(3, i)
        self.copy(6, i).start()

    def finish(self):
        for i in self.every():
            for k in (0, 4, 5, 6):
                self.arrived(k, i)

    def drain(self):
        for i in self.every():
            for k in range(7):
                self.copy(k, i).wait_send()


PARTNER, PRIM, SEC = 0, 1, 2


def fill_table(routing, me, out):
    out[...] = jnp.zeros((32, 128), F32)
    for layer in range(2):
        experts, slots, gates = (routing[3 * layer + k] for k in range(3))
        keys = jnp.where(slots[...] >= 0, experts[...] * HALF_ROWS + (me % 4) * CAP + slots[...], -1)
        out[16 * layer : 16 * layer + 8, 0:TOK] = keys.astype(F32)
        out[16 * layer + 8 : 16 * layer + 16, 0:TOK] = gates[...]


def join_table(tab, table):
    low = lax.broadcasted_iota(jnp.int32, (32, 128), 1) < TOK
    for p in range(4):
        table[:, p * 128 : (p + 1) * 128] = jnp.where(low, tab[2 * p], pltpu.roll(tab[2 * p + 1], TOK, 1))


def build_onehot(table, base, me, onehot, gate_col):
    for h in range(2):
        cols = slice(h * 256, (h + 1) * 256)
        keys = [table[base + j : base + j + 1, cols] for j in range(8)]
        gates = [table[base + 8 + j : base + 9 + j, cols] for j in range(8)]
        for e in range(LOCAL):
            row = (lax.broadcasted_iota(jnp.int32, (HALF_ROWS, 256), 0) + (e + me * LOCAL) * HALF_ROWS).astype(F32)
            gate = jnp.zeros((HALF_ROWS, 256), F32)
            hit = jnp.zeros((HALF_ROWS, 256), F32)
            for j in range(8):
                match = row == keys[j]
                gate = jnp.where(match, gates[j], gate)
                hit = jnp.where(match, 1.0, hit)
            onehot[h, e * HALF_ROWS : (e + 1) * HALF_ROWS, :] = hit.astype(BF16)
            gate_col[h, e * HALF_ROWS : (e + 1) * HALF_ROWS, :] = jnp.broadcast_to(jnp.sum(gate, axis=1, keepdims=True), (HALF_ROWS, 128))


def take_rows(onehot, tokens, rows, gate_col=None):
    for h in range(2):
        for n in range(D // STEP):
            cols = slice(n * STEP, (n + 1) * STEP)
            out = jnp.dot(onehot[h], tokens[h * 256 : (h + 1) * 256, cols], preferred_element_type=F32)
            if gate_col is not None:
                out = out * gate_col[h, :, 0:1]
            out = out.astype(BF16)
            for e in range(LOCAL):
                rows[e, h * HALF_ROWS : (h + 1) * HALF_ROWS, cols] = out[e * HALF_ROWS : (e + 1) * HALF_ROWS]


def forward_expert(e, u, w1, w3, a, b, hid):
    act = jnp.dot(u[e], w1[e], preferred_element_type=F32).astype(BF16)
    up = jnp.dot(u[e], w3[e], preferred_element_type=F32).astype(BF16)
    a[e] = act
    b[e] = up
    wide = act.astype(F32)
    hid[e] = (wide * jax.nn.sigmoid(wide) * up.astype(F32)).astype(BF16)


TRANS_B = (((1,), (1,)), ((), ()))
TRANS_A = (((0,), (0,)), ((), ()))


def hidden_grads(e, z, w2, a, b):
    dh = lax.dot_general(z[e], w2[e], TRANS_B, preferred_element_type=F32)
    act = a[e].astype(F32)
    up = b[e].astype(F32)
    sig = jax.nn.sigmoid(act)
    a[e] = (dh * up * sig * (1.0 + act * (1.0 - sig))).astype(BF16)
    b[e] = (dh * (act * sig)).astype(BF16)


def row_grads(e, cols, w1, w3, a, b, dxr):
    dx = lax.dot_general(a[e], w1[e, cols, :], TRANS_B, preferred_element_type=F32) + lax.dot_general(b[e], w3[e, cols, :], TRANS_B, preferred_element_type=F32)
    dx = dx.astype(BF16)
    for h in range(2):
        dxr[h, e * HALF_ROWS : (e + 1) * HALF_ROWS, cols] = dx[h * HALF_ROWS : (h + 1) * HALF_ROWS]


def return_sums(ids, core, x, y, onehot, w1, w3, a, b, dxr, sums, inbox, send, recv, ssem, outs, between):
    def exchange(n, yy, xx):
        theirs = 4 * yy + 2 * xx + (1 - core)
        cols = pl.ds(n * STEP, STEP)
        src = sums.at[pl.ds(pl.multiple_of(theirs * TOK, TOK), TOK), cols]
        return pltpu.make_async_remote_copy(src_ref=src, dst_ref=inbox.at[2 * yy + xx, :, cols], send_sem=send.at[n, 2 * yy + xx], recv_sem=recv.at[n, 2 * yy + xx], device_id={"expert": ids["partner"]}, device_id_type=MESH)

    def store(n, name, xx, yy, out, k):
        cols = pl.ds(n * STEP, STEP)
        return pltpu.make_async_copy(inbox.at[2 * yy + xx, :, cols], out.at[:, cols], ssem.at[n, k])

    blocks = (("me", x, y, outs[0], 0), ("x", 1 - x, y, outs[1], 1), ("y", x, 1 - y, outs[2], 2), ("diag", 1 - x, 1 - y, outs[3], 3))

    def collect(n):
        for k in range(4):
            exchange(n, k // 2, k % 2).wait_recv()
        cols = slice(n * STEP, (n + 1) * STEP)
        for name, xx, yy, out, k in blocks:
            inbox[2 * yy + xx, :, cols] = inbox[2 * yy + xx, :, cols] + sums[pl.ds(pl.multiple_of(ids[name] * TOK, TOK), TOK), cols]
            store(n, name, xx, yy, out, k).start()

    for n in range(D // STEP):
        cols = slice(n * STEP, (n + 1) * STEP)
        for e in range(LOCAL):
            row_grads(e, cols, w1, w3, a, b, dxr)
        for h in range(2):
            sums[h * 256 : (h + 1) * 256, cols] = lax.dot_general(onehot[h], dxr[h, :, cols], TRANS_A, preferred_element_type=F32)
        for k in range(4):
            exchange(n, k // 2, k % 2).start()
        if n > 0:
            collect(n - 1)
        between(n)
    collect(D // STEP - 1)
    for n in range(D // STEP):
        for k in range(4):
            exchange(n, k // 2, k % 2).wait_send()
        for entry in blocks:
            store(n, *entry).wait()


class Weights:
    def __init__(self, hbm, vmem, sems):
        self.hbm, self.vmem, self.sems = hbm, vmem, sems

    def copy(self, k, e):
        return pltpu.make_async_copy(self.hbm[k].at[e], self.vmem[k].at[e], self.sems.at[k, e])

    def start(self, kinds, experts):
        for e in experts:
            for k in kinds:
                self.copy(k, e).start()

    def wait(self, kinds, e):
        for k in kinds:
            self.copy(k, e).wait()


def layer_two_kernel(*refs):
    routing_h, refs = refs[:6], refs[6:]
    (y_h, dy_h, x_h, w1_h, w3_h, w2_h,
     u_o, z_o, hid_o, da_o, db_o, xall_o, table_o, s_me, s_x, s_y, s_d) = refs[:17]
    routing, refs = refs[17:23], refs[23:]
    (tab, yall, dall, xall, w1, w3, w2, onehot, gate_col, u, z, a, b, hid, dxr, sums, inbox,
     lsem, wsem, osem, tsend, trecv, gsend, grecv, xsend, xrecv, ssem) = refs
    ids, core, x, y = place()
    small = [pltpu.make_async_copy(src, dst, lsem.at[3 + i]) for i, (src, dst) in enumerate(zip(routing_h, routing))]
    local = [pltpu.make_async_copy(src, block(dst, ids["me"]), lsem.at[i]) for i, (src, dst) in enumerate(((y_h, yall), (dy_h, dall), (x_h, xall)))]
    for c in small + local:
        c.start()
    for c in small:
        c.wait()
    fill_table(routing, ids["me"], tab.at[ids["me"]])
    for c in local:
        c.wait()
    weights = Weights((w1_h, w3_h, w2_h), (w1, w3, w2), wsem)
    weights.start((0, 1, 2), range(LOCAL))
    barrier(ids)
    gt = Gather(ids, tab, tsend, trecv, 0)
    gy, gd, gx = [Gather(ids, ref, gsend.at[i], grecv.at[i], 2) for i, ref in enumerate((yall, dall, xall))]
    for k in (PRIM, SEC, PARTNER):
        gt.start(k)
    for k in (PRIM, SEC, PARTNER):
        gy.start(k)
    for k in (PRIM, PARTNER):
        gd.start(k)
    gt.relay_prim(0)
    gy.relay_prim(0)
    gt.relay_rest(0)
    gt.finish()
    gy.relay_prim(1)
    gd.start(SEC)
    join_table(tab, table_o)
    build_onehot(table_o, 0, ids["me"], onehot, gate_col)
    gy.relay_rest(0)
    gy.relay_rest(1)
    gy.finish()
    take_rows(onehot, yall, u)
    store_u = pltpu.make_async_copy(u, u_o, osem.at[0])
    store_u.start()

    def forward(first, last):
        for e in range(first, last):
            weights.wait((0, 1), e)
            forward_expert(e, u, w1, w3, a, b, hid)

    forward(0, 1)
    gd.relay_prim(0)
    gd.relay_prim(1)
    for k in (PRIM, SEC, PARTNER):
        gx.start(k)
    forward(1, LOCAL)
    gd.relay_rest(0)
    gd.relay_rest(1)
    gd.finish()
    take_rows(onehot, dall, z, gate_col)
    gx.relay_prim(0)
    store_z = pltpu.make_async_copy(z, z_o, osem.at[1])
    store_h = pltpu.make_async_copy(hid, hid_o, osem.at[2])
    store_z.start()
    store_h.start()
    for e in range(LOCAL):
        weights.wait((2,), e)
        hidden_grads(e, z, w2, a, b)
    gx.relay_prim(1)
    store_a = pltpu.make_async_copy(a, da_o, osem.at[3])
    store_b = pltpu.make_async_copy(b, db_o, osem.at[4])
    store_a.start()
    store_b.start()
    store_x = pltpu.make_async_copy(xall, xall_o, osem.at[5])

    def between(n):
        if n == 0:
            gx.relay_rest(0)
            gx.relay_rest(1)
        if n == 1:
            gx.finish()
            store_x.start()

    return_sums(ids, core, x, y, onehot, w1, w3, a, b, dxr, sums, inbox, xsend, xrecv, ssem, (s_me, s_x, s_y, s_d), between)
    for g in (gt, gy, gd, gx):
        g.drain()
    for c in (store_u, store_z, store_h, store_a, store_b, store_x):
        c.wait()


def layer_one_kernel(dy_h, r_me, r_x, r_y, r_d, table, xall_h, w1_h, w3_h, w2_h,
                     u_o, z_o, hid_o, da_o, db_o, dy1_o, s_me, s_x, s_y, s_d,
                     dall, xall, w1, w3, w2, onehot, gate_col, u, z, a, b, hid, dxr, sums, inbox,
                     lsem, wsem, osem, gsend, grecv, xsend, xrecv, ssem):
    ids, core, x, y = place()
    load_x = pltpu.make_async_copy(xall_h, xall, lsem.at[0])
    load_x.start()
    weights = Weights((w1_h, w3_h, w2_h), (w1, w3, w2), wsem)
    dy1 = (dy_h[...].astype(F32) + ((r_me[...] + r_x[...]) + (r_y[...] + r_d[...]))).astype(BF16)
    dall[pl.ds(pl.multiple_of(ids["me"] * TOK, TOK), TOK), :] = dy1
    dy1_o[...] = dy1
    barrier(ids)
    gd = Gather(ids, dall, gsend, grecv, 2)
    for k in (PRIM, SEC, PARTNER):
        gd.start(k)
    load_x.wait()
    weights.start((0, 1), (0, 1))
    build_onehot(table, 16, ids["me"], onehot, gate_col)
    weights.start((0, 1), (2, 3, 4))
    take_rows(onehot, xall, u)
    weights.start((2,), range(LOCAL))
    store_u = pltpu.make_async_copy(u, u_o, osem.at[0])
    store_u.start()

    def forward(first, last):
        for e in range(first, last):
            weights.wait((0, 1), e)
            forward_expert(e, u, w1, w3, a, b, hid)

    forward(0, 1)
    gd.relay_prim(0)
    forward(1, 2)
    gd.relay_prim(1)
    forward(2, LOCAL)
    gd.relay_rest(0)
    gd.relay_rest(1)
    gd.finish()
    take_rows(onehot, dall, z, gate_col)
    store_z = pltpu.make_async_copy(z, z_o, osem.at[1])
    store_h = pltpu.make_async_copy(hid, hid_o, osem.at[2])
    store_z.start()
    store_h.start()
    for e in range(LOCAL):
        weights.wait((2,), e)
        hidden_grads(e, z, w2, a, b)
    store_a = pltpu.make_async_copy(a, da_o, osem.at[3])
    store_b = pltpu.make_async_copy(b, db_o, osem.at[4])
    store_a.start()
    store_b.start()
    return_sums(ids, core, x, y, onehot, w1, w3, a, b, dxr, sums, inbox, xsend, xrecv, ssem, (s_me, s_x, s_y, s_d), lambda n: None)
    gd.drain()
    for c in (store_u, store_z, store_h, store_a, store_b):
        c.wait()


HBM_SPEC = pl.BlockSpec(memory_space=pl.ANY)
VMEM_SPEC = pl.BlockSpec(memory_space=pltpu.VMEM)


def compute_scratch():
    return [
        pltpu.VMEM((LOCAL, D, F), BF16), pltpu.VMEM((LOCAL, D, F), BF16), pltpu.VMEM((LOCAL, F, D), BF16),
        pltpu.VMEM((2, LOCAL * HALF_ROWS, 256), BF16), pltpu.VMEM((2, LOCAL * HALF_ROWS, 128), F32),
        pltpu.VMEM((LOCAL, ROWS, D), BF16), pltpu.VMEM((LOCAL, ROWS, D), BF16),
        pltpu.VMEM((LOCAL, ROWS, F), BF16), pltpu.VMEM((LOCAL, ROWS, F), BF16), pltpu.VMEM((LOCAL, ROWS, F), BF16),
        pltpu.VMEM((2, LOCAL * HALF_ROWS, D), BF16), pltpu.VMEM((8 * TOK, D), F32), pltpu.VMEM((4, TOK, D), F32),
    ]


ROW_OUTS = [jax.ShapeDtypeStruct((LOCAL, ROWS, D), BF16)] * 2 + [jax.ShapeDtypeStruct((LOCAL, ROWS, F), BF16)] * 3
SUM_OUTS = [jax.ShapeDtypeStruct((TOK, D), F32)] * 4
DMA = pltpu.SemaphoreType.DMA


def layer_two(routing, y_mid, dy_out, x_tokens, w1, w3, w2):
    all_tok = pltpu.VMEM((8 * TOK, D), BF16)
    table_in = [pltpu.VMEM((8, TOK), t) for t in (jnp.int32, jnp.int32, F32)]
    return pl.pallas_call(
        layer_two_kernel, name="layer_two",
        out_shape=ROW_OUTS + [jax.ShapeDtypeStruct((8 * TOK, D), BF16), jax.ShapeDtypeStruct((32, 8 * TOK), F32)] + SUM_OUTS,
        in_specs=[HBM_SPEC] * 12, out_specs=[HBM_SPEC] * 6 + [VMEM_SPEC] + [HBM_SPEC] * 4,
        scratch_shapes=table_in * 2 + [pltpu.VMEM((8, 32, 128), F32), all_tok, all_tok, all_tok] + compute_scratch()
        + [DMA((9,)), DMA((3, LOCAL)), DMA((6,)), DMA((1, 7)), DMA((1, 7)), DMA((3, 2, 7)), DMA((3, 2, 7)), DMA((3, 4)), DMA((3, 4)), DMA((3, 4))],
        compiler_params=pltpu.CompilerParams(collective_id=0, has_side_effects=True, vmem_limit_bytes=56 * 2**20),
        cost_estimate=pl.CostEstimate(flops=16 * 10**9, bytes_accessed=36 * 2**20, transcendentals=0),
    )(*routing, y_mid, dy_out, x_tokens, w1, w3, w2)


def layer_one(dy_out, returned, table, xall, w1, w3, w2):
    all_tok = pltpu.VMEM((8 * TOK, D), BF16)
    return pl.pallas_call(
        layer_one_kernel, name="layer_one",
        out_shape=ROW_OUTS + [jax.ShapeDtypeStruct((TOK, D), BF16)] + SUM_OUTS,
        in_specs=[VMEM_SPEC] * 6 + [HBM_SPEC] * 4, out_specs=[HBM_SPEC] * 5 + [VMEM_SPEC] + [HBM_SPEC] * 4,
        scratch_shapes=[all_tok, all_tok] + compute_scratch()
        + [DMA((1,)), DMA((3, LOCAL)), DMA((5,)), DMA((2, 7)), DMA((2, 7)), DMA((3, 4)), DMA((3, 4)), DMA((3, 4))],
        compiler_params=pltpu.CompilerParams(collective_id=1, has_side_effects=True, vmem_limit_bytes=50 * 2**20),
        cost_estimate=pl.CostEstimate(flops=16 * 10**9, bytes_accessed=36 * 2**20, transcendentals=0),
    )(dy_out, *returned, table, xall, w1, w3, w2)


PARTS = 4


def weight_grad_kernel(u_h, z_h, hid_h, da_h, db_h, dw1_h, dw3_h, dw2_h, u, z, hid, da, db, ring1, ring3, ring2, isem, osem):
    def load(e):
        return [pltpu.make_async_copy(src.at[e], dst.at[e], isem.at[k, e]) for k, (src, dst) in enumerate(((u_h, u), (da_h, da), (db_h, db), (hid_h, hid), (z_h, z)))]

    for e in range(LOCAL):
        for c in load(e):
            c.start()

    def store(e, p):
        rows, cols = D // PARTS, F // PARTS
        return [pltpu.make_async_copy(ring1.at[p], dw1_h.at[e, pl.ds(p * rows, rows)], osem.at[0, p]),
                pltpu.make_async_copy(ring3.at[p], dw3_h.at[e, pl.ds(p * rows, rows)], osem.at[1, p]),
                pltpu.make_async_copy(ring2.at[p], dw2_h.at[e, pl.ds(p * cols, cols)], osem.at[2, p])]

    def expert(e, carry):
        for c in load(e):
            c.wait()
        for p in range(PARTS):
            rows, cols = slice(p * (D // PARTS), (p + 1) * (D // PARTS)), slice(p * (F // PARTS), (p + 1) * (F // PARTS))
            out = store(e, p)

            @pl.when(e > 0)
            def _():
                for c in out:
                    c.wait()

            ring1[p] = lax.dot_general(u[e, :, rows], da[e], TRANS_A, preferred_element_type=F32)
            out[0].start()
            ring3[p] = lax.dot_general(u[e, :, rows], db[e], TRANS_A, preferred_element_type=F32)
            out[1].start()
            ring2[p] = lax.dot_general(hid[e, :, cols], z[e], TRANS_A, preferred_element_type=F32)
            out[2].start()
        return carry

    lax.fori_loop(0, LOCAL, expert, 0)
    for p in range(PARTS):
        for c in store(LOCAL - 1, p):
            c.wait()


def weight_grads(u, z, hid, da, db):
    wide, narrow = pltpu.VMEM((LOCAL, ROWS, D), BF16), pltpu.VMEM((LOCAL, ROWS, F), BF16)
    ring = pltpu.VMEM((PARTS, D // PARTS, F), F32)
    return pl.pallas_call(
        weight_grad_kernel, name="weight_grads",
        in_specs=[HBM_SPEC] * 5, out_specs=[HBM_SPEC] * 3,
        out_shape=[jax.ShapeDtypeStruct((LOCAL, D, F), F32)] * 2 + [jax.ShapeDtypeStruct((LOCAL, F, D), F32)],
        scratch_shapes=[wide, wide, narrow, narrow, narrow, ring, ring, pltpu.VMEM((PARTS, F // PARTS, D), F32), DMA((5, LOCAL)), DMA((3, PARTS))],
        compiler_params=pltpu.CompilerParams(vmem_limit_bytes=60 * 2**20),
        cost_estimate=pl.CostEstimate(flops=18 * 10**9, bytes_accessed=56 * 2**20, transcendentals=0),
    )(u, z, hid, da, db)


def exchange_sums(sums):
    swap = lambda mask: [(i, i ^ mask) for i in range(8)]
    return (sums[0],) + tuple(lax.ppermute(sums[k], "expert", swap(mask)) for k, mask in ((1, 2), (2, 4), (3, 6)))


def solution(mesh):
    tok_spec = P(("data", "expert"), None)
    weight_spec = P("expert", None, None)
    grad_spec = P(("data", "expert"), None, None)

    def local_step(x_tokens, y_mid, dy_out, experts_one, gates_one, slots_one, experts_two, gates_two, slots_two, w_gate_one, w_up_one, w_down_one, w_gate_two, w_up_two, w_down_two):
        routing = [r.T for r in (experts_two, slots_two, gates_two, experts_one, slots_one, gates_one)]
        *rows_two, xall, table, s0, s1, s2, s3 = layer_two(routing, y_mid, dy_out, x_tokens, w_gate_two, w_up_two, w_down_two)
        returned = exchange_sums((s0, s1, s2, s3))
        grads_two = weight_grads(*rows_two)
        *rows_one, dy_mid, s0, s1, s2, s3 = layer_one(dy_out, returned, table, xall, w_gate_one, w_up_one, w_down_one)
        r = exchange_sums((s0, s1, s2, s3))
        grads_one = weight_grads(*rows_one)
        dx_tokens = (dy_mid.astype(F32) + ((r[0] + r[1]) + (r[2] + r[3]))).astype(BF16)
        return (dx_tokens, *grads_one, *grads_two)

    return jax.shard_map(local_step, mesh=mesh, in_specs=(tok_spec,) * 9 + (weight_spec,) * 6, out_specs=(tok_spec,) + (grad_spec,) * 6, check_vma=False)
```

```python
import functools
import jax
import jax.numpy as jnp
from jax import lax
from jax.experimental import pallas as pl
from jax.experimental.pallas import tpu as pltpu
from jax.sharding import PartitionSpec as P

MESH = pl.DeviceIdType.MESH
F32 = jnp.float32
BF16 = jnp.bfloat16
CAP = 24
LOCAL = 5
D = 1536
F = 512
TOK = 64
HALF_ROWS = 4 * CAP
ROWS = 8 * CAP
STEP = 512
SLOTS = 512
CHUNKS = ((0, 768), (768, 512), (1280, 256))


def place():
    me = lax.axis_index("expert")
    core, x, y = me % 2, (me // 2) % 2, me // 4
    ident = lambda xx, yy, cc: 4 * yy + 2 * xx + cc
    ids = {
        "me": me,
        "partner": ident(x, y, 1 - core),
        "x": ident(1 - x, y, core),
        "y": ident(x, 1 - y, core),
        "diag": ident(1 - x, 1 - y, core),
        "prim": ident(x + (1 - core) * (1 - 2 * x), y + core * (1 - 2 * y), core),
        "sec": ident(x + core * (1 - 2 * x), y + (1 - core) * (1 - 2 * y), core),
        "p_prim": ident(x + core * (1 - 2 * x), y + (1 - core) * (1 - 2 * y), 1 - core),
        "p_sec": ident(x + (1 - core) * (1 - 2 * x), y + core * (1 - 2 * y), 1 - core),
        "p_diag": ident(1 - x, 1 - y, 1 - core),
    }
    return ids, core, x, y


def greet(ids):
    for peer in ("partner", "x", "y"):
        pl.semaphore_signal(pltpu.get_barrier_semaphore(), inc=1, device_id={"expert": ids[peer]}, device_id_type=MESH)


def await_peers():
    pl.semaphore_wait(pltpu.get_barrier_semaphore(), 3)


def block(ref, ident):
    return ref.at[pl.ds(pl.multiple_of(ident * TOK, TOK), TOK)]


class Gather:
    ROUTES = (("me", "partner"), ("me", "prim"), ("me", "sec"), ("prim", "sec"), ("prim", "partner"), ("sec", "partner"), ("diag", "partner"))
    ARRIVE = ("partner", "prim", "sec", "diag", "p_prim", "p_sec", "p_diag")

    def __init__(self, ids, ref, send, recv, pieces):
        self.ids, self.ref, self.send, self.recv, self.pieces = ids, ref, send, recv, pieces

    def part(self, ident, i):
        if self.pieces == 0:
            return self.ref.at[ident]
        size = TOK // self.pieces
        return self.ref.at[pl.ds(pl.multiple_of(ident * TOK + i * size, size), size)]

    def arrival(self, k, i):
        return self.recv.at[3 * i + k - 1] if 1 <= k <= 3 else self.recv.at[3 * max(self.pieces, 1)]

    def copy(self, k, i, what=None, where=None):
        what, where = what or self.ROUTES[k][0], where or self.ROUTES[k][1]
        part = self.part(self.ids[what], i)
        return pltpu.make_async_remote_copy(src_ref=part, dst_ref=part, send_sem=self.send.at[0], recv_sem=self.arrival(k, i), device_id={"expert": self.ids[where]}, device_id_type=MESH)

    def arrived(self, k, i):
        self.copy(k, i, self.ARRIVE[k], "partner").wait_recv()

    def every(self):
        return range(max(self.pieces, 1))

    def start(self, k):
        for i in self.every():
            self.copy(k, i).start()

    def relay_prim(self, i):
        self.arrived(1, i)
        self.copy(3, i).start()
        self.copy(4, i).start()

    def relay_rest(self, i):
        self.arrived(2, i)
        self.copy(5, i).start()
        self.arrived(3, i)
        self.copy(6, i).start()

    def blocks(self, count):
        part = self.ref.at[pl.ds(0, count * (TOK if self.pieces else 1))]
        return pltpu.make_async_remote_copy(src_ref=part, dst_ref=part, send_sem=self.send.at[0], recv_sem=self.recv.at[3 * max(self.pieces, 1)], device_id={"expert": self.ids["partner"]}, device_id_type=MESH)

    def finish(self):
        self.blocks(4).wait_recv()

    def drain(self):
        self.blocks(7).wait_send()


PARTNER, PRIM, SEC = 0, 1, 2


def fill_table(routing, me, out):
    out[...] = jnp.zeros((32, 128), F32)
    for layer in range(2):
        experts, slots, gates = (routing[3 * layer + k] for k in range(3))
        keys = jnp.where(slots[...] >= 0, experts[...] * HALF_ROWS + (me % 4) * CAP + slots[...], -1)
        out[16 * layer : 16 * layer + 8, 0:TOK] = keys.astype(F32)
        out[16 * layer + 8 : 16 * layer + 16, 0:TOK] = gates[...]


def join_table(tab, table):
    low = lax.broadcasted_iota(jnp.int32, (32, 128), 1) < TOK
    for p in range(4):
        table[:, p * 128 : (p + 1) * 128] = jnp.where(low, tab[2 * p], pltpu.roll(tab[2 * p + 1], TOK, 1))


def build_onehot(table, base, me, onehot, gate_col):
    for h in range(2):
        onehot[h, LOCAL * HALF_ROWS : SLOTS, :] = jnp.zeros((SLOTS - LOCAL * HALF_ROWS, 256), BF16)
        cols = slice(h * 256, (h + 1) * 256)
        keys = [table[base + j : base + j + 1, cols] for j in range(8)]
        gates = [table[base + 8 + j : base + 9 + j, cols] for j in range(8)]
        for e in range(LOCAL):
            row = (lax.broadcasted_iota(jnp.int32, (HALF_ROWS, 256), 0) + (e + me * LOCAL) * HALF_ROWS).astype(F32)
            gate = jnp.zeros((HALF_ROWS, 256), F32)
            hit = jnp.zeros((HALF_ROWS, 256), F32)
            for j in range(8):
                match = row == keys[j]
                gate = jnp.where(match, gates[j], gate)
                hit = jnp.where(match, 1.0, hit)
            onehot[h, e * HALF_ROWS : (e + 1) * HALF_ROWS, :] = hit.astype(BF16)
            gate_col[h, e * HALF_ROWS : (e + 1) * HALF_ROWS, :] = jnp.broadcast_to(jnp.sum(gate, axis=1, keepdims=True), (HALF_ROWS, 128))


def build_scatter(onehot, scatter):
    for h in range(2):
        scatter[h] = jnp.transpose(onehot[h])


def turn_tall(src, dst, e):
    for n in range(D // 128):
        dst[e, :, n * 128 : (n + 1) * 128] = jnp.transpose(src[e, n * 128 : (n + 1) * 128, :])


def turn_wide(src, dst, e):
    for n in range(D // 128):
        dst[e, n * 128 : (n + 1) * 128, :] = jnp.transpose(src[e, :, n * 128 : (n + 1) * 128])


def take_rows(onehot, tokens, rows, gate_col=None):
    for h in range(2):
        for n in range(D // STEP):
            cols = slice(n * STEP, (n + 1) * STEP)
            out = jnp.dot(onehot[h, 0 : LOCAL * HALF_ROWS], tokens[h * 256 : (h + 1) * 256, cols], preferred_element_type=F32)
            if gate_col is not None:
                out = out * gate_col[h, :, 0:1]
            out = out.astype(BF16)
            for e in range(LOCAL):
                rows[e, h * HALF_ROWS : (h + 1) * HALF_ROWS, cols] = out[e * HALF_ROWS : (e + 1) * HALF_ROWS]


def forward_expert(e, u, w1, w3, a, b, hid):
    act = jnp.dot(u[e], w1[e], preferred_element_type=F32).astype(BF16)
    up = jnp.dot(u[e], w3[e], preferred_element_type=F32).astype(BF16)
    a[e] = act
    b[e] = up
    wide = act.astype(F32)
    hid[e] = (wide * jax.nn.sigmoid(wide) * up.astype(F32)).astype(BF16)


TRANS_B = (((1,), (1,)), ((), ()))
TRANS_A = (((0,), (0,)), ((), ()))


def hidden_grads(e, z, w2, a, b):
    dh = jnp.dot(z[e], w2[e], preferred_element_type=F32)
    act = a[e].astype(F32)
    up = b[e].astype(F32)
    sig = jax.nn.sigmoid(act)
    a[e] = (dh * up * sig * (1.0 + act * (1.0 - sig))).astype(BF16)
    b[e] = (dh * (act * sig)).astype(BF16)


def row_grads(e, cols, turned, w1, w3, a, b, dxr):
    if turned:
        dx = jnp.dot(a[e], w1[e, :, cols], preferred_element_type=F32) + jnp.dot(b[e], w3[e, :, cols], preferred_element_type=F32)
    else:
        dx = lax.dot_general(a[e], w1[e, cols, :], TRANS_B, preferred_element_type=F32) + lax.dot_general(b[e], w3[e, cols, :], TRANS_B, preferred_element_type=F32)
    dx = dx.astype(BF16)
    for h in range(2):
        dxr[e * HALF_ROWS : (e + 1) * HALF_ROWS, h * (D // 2) : h * (D // 2) + dx.shape[1]] = dx[h * HALF_ROWS : (h + 1) * HALF_ROWS]


def return_sums(ids, core, x, y, scatter, turned, w1, w3, a, b, dxr, sums, inbox, send, recv, ssem, outs, between):
    def exchange(n, yy, xx):
        theirs = 4 * yy + 2 * xx + (1 - core)
        cols = pl.ds(*CHUNKS[n])
        src = sums.at[pl.ds(pl.multiple_of(theirs * TOK, TOK), TOK), cols]
        return pltpu.make_async_remote_copy(src_ref=src, dst_ref=inbox.at[2 * yy + xx, :, cols], send_sem=send.at[0], recv_sem=recv.at[n], device_id={"expert": ids["partner"]}, device_id_type=MESH)

    def whole(ref, sem):
        return pltpu.make_async_remote_copy(src_ref=ref, dst_ref=ref, send_sem=send.at[0], recv_sem=sem, device_id={"expert": ids["partner"]}, device_id_type=MESH)

    def store(n, name, xx, yy, out, k):
        cols = pl.ds(*CHUNKS[n])
        return pltpu.make_async_copy(inbox.at[2 * yy + xx, :, cols], out.at[:, cols], ssem.at[k])

    blocks = (("me", x, y, outs[0], 0), ("x", 1 - x, y, outs[1], 1), ("y", x, 1 - y, outs[2], 2), ("diag", 1 - x, 1 - y, outs[3], 3))

    def collect(n):
        cols = slice(CHUNKS[n][0], sum(CHUNKS[n]))
        whole(inbox.at[:, :, cols], recv.at[n]).wait_recv()
        for name, xx, yy, out, k in blocks:
            inbox[2 * yy + xx, :, cols] = inbox[2 * yy + xx, :, cols] + sums[pl.ds(pl.multiple_of(ids[name] * TOK, TOK), TOK), cols]
            store(n, name, xx, yy, out, k).start()

    for n in range(len(CHUNKS)):
        cols = slice(CHUNKS[n][0], sum(CHUNKS[n]))
        for e in range(LOCAL):
            row_grads(e, cols, turned, w1, w3, a, b, dxr)
        for h in range(2):
            sums[h * 256 : (h + 1) * 256, cols] = jnp.dot(scatter[h, :, 0 : LOCAL * HALF_ROWS], dxr[0 : LOCAL * HALF_ROWS, h * (D // 2) : h * (D // 2) + CHUNKS[n][1]], preferred_element_type=F32)
        for k in range(4):
            exchange(n, k // 2, k % 2).start()
        if n == 2:
            collect(0)
        between(n)
    collect(1)
    collect(2)
    whole(inbox, recv.at[0]).wait_send()
    for name, xx, yy, out, k in blocks:
        pltpu.make_async_copy(inbox.at[2 * yy + xx], out, ssem.at[k]).wait()


class Weights:
    def __init__(self, hbm, vmem, sems):
        self.hbm, self.vmem, self.sems = hbm, vmem, sems

    def copy(self, k, e):
        return pltpu.make_async_copy(self.hbm[k].at[e], self.vmem[k].at[e], self.sems.at[k, e])

    def start(self, kinds, experts):
        for e in experts:
            for k in kinds:
                self.copy(k, e).start()

    def wait(self, kinds, e):
        for k in kinds:
            self.copy(k, e).wait()


def layer_two_kernel(*refs):
    routing_h, refs = refs[:6], refs[6:]
    (y_h, dy_h, x_h, w1_h, w3_h, w2_h,
     u_o, z_o, hid_o, da_o, db_o, xall_o, table_o, s_me, s_x, s_y, s_d) = refs[:17]
    routing, refs = refs[17:23], refs[23:]
    (tab, yall, dall, xall, w1, w3, w2, onehot, scatter, gate_col, w2t, u, z, a, b, hid, sums, inbox, w3t, table,
     lsem, wsem, osem, tsend, trecv, gsend, grecv, xsend, xrecv, ssem) = refs
    ids, core, x, y = place()
    greet(ids)
    small = [pltpu.make_async_copy(src, dst, lsem.at[3 + i]) for i, (src, dst) in enumerate(zip(routing_h, routing))]
    local = [pltpu.make_async_copy(src, block(dst, ids["me"]), lsem.at[i]) for i, (src, dst) in enumerate(((y_h, yall), (dy_h, dall), (x_h, xall)))]
    for c in small + local:
        c.start()
    for c in small:
        c.wait()
    fill_table(routing, ids["me"], tab.at[ids["me"]])
    local[0].wait()
    weights = Weights((w1_h, w3_h, w2_h), (w1, w3, w2), wsem)
    gt = Gather(ids, tab, tsend, trecv, 0)
    gy, gd, gx = [Gather(ids, ref, gsend.at[i], grecv.at[i], 2) for i, ref in enumerate((yall, dall, xall))]
    await_peers()
    gt.start(PRIM)
    gt.start(SEC)
    gy.start(PRIM)
    gt.start(PARTNER)
    for c in local[1:]:
        c.wait()
    weights.start((2,), range(LOCAL))
    weights.start((0, 1), range(LOCAL))

    def turn(first, last):
        for i in range(first, last):
            e = i % LOCAL
            if i < 2 * LOCAL:
                weights.wait(((2,), (0,))[i // LOCAL], e)
            (turn_wide, turn_tall, turn_tall)[i // LOCAL]((w2, w1, w3)[i // LOCAL], (w2t, w2, w3t)[i // LOCAL], e)

    turn(0, 1)
    gy.start(PARTNER)
    turn(1, 2)
    gy.start(SEC)
    turn(2, 3)
    gt.relay_prim(0)
    gy.relay_prim(0)
    turn(3, 5)
    gy.relay_prim(1)
    turn(5, 8)
    gd.start(PRIM)
    gt.relay_rest(0)
    turn(8, 9)
    gt.finish()
    join_table(tab, table)
    save_table = pltpu.make_async_copy(table, table_o, osem.at[6])
    save_table.start()
    build_onehot(table, 0, ids["me"], onehot, gate_col)
    gd.start(SEC)
    gd.start(PARTNER)
    gy.relay_rest(0)
    build_scatter(onehot, scatter)
    turn(9, 10)
    gy.relay_rest(1)
    for e in range(LOCAL):
        weights.wait((1,), e)
    turn(10, 11)
    gy.finish()
    gd.relay_prim(0)
    take_rows(onehot, yall, u)
    store_u = pltpu.make_async_copy(u, u_o, osem.at[0])
    store_u.start()

    def forward(first, last):
        lax.fori_loop(first, last, lambda e, carry: (forward_expert(e, u, w1, w3, a, b, hid), carry)[1], 0)

    gd.relay_prim(1)
    forward(0, 2)
    gx.start(PRIM)
    forward(2, 4)
    gx.start(SEC)
    forward(4, LOCAL)
    gd.relay_rest(0)
    turn(11, 13)
    gd.relay_rest(1)
    turn(13, 3 * LOCAL)
    gx.relay_prim(0)
    gd.finish()
    gx.start(PARTNER)
    take_rows(onehot, dall, z, gate_col)
    store_z = pltpu.make_async_copy(z, z_o, osem.at[1])
    store_h = pltpu.make_async_copy(hid, hid_o, osem.at[2])
    store_z.start()
    store_h.start()
    gx.relay_prim(1)
    for e in range(LOCAL):
        hidden_grads(e, z, w2t, a, b)
    store_a = pltpu.make_async_copy(a, da_o, osem.at[3])
    store_b = pltpu.make_async_copy(b, db_o, osem.at[4])
    store_a.start()
    store_b.start()
    store_x = pltpu.make_async_copy(xall, xall_o, osem.at[5])

    def between(n):
        if n == 1:
            gx.relay_rest(0)
            gx.relay_rest(1)
        if n == 2:
            gx.finish()
            store_x.start()

    gy.drain()
    return_sums(ids, core, x, y, scatter, True, w2, w3t, a, b, yall, sums, inbox, xsend, xrecv, ssem, (s_me, s_x, s_y, s_d), between)
    for g in (gt, gd, gx):
        g.drain()
    for c in (store_u, store_z, store_h, store_a, store_b, store_x, save_table):
        c.wait()


def layer_one_kernel(dy_h, r_me, r_x, r_y, r_d, table, xall_h, w1_h, w3_h, w2_h,
                     u_o, z_o, hid_o, da_o, db_o, dy1_o, s_me, s_x, s_y, s_d,
                     dall, xall, w1, w3, w2, onehot, scatter, gate_col, w2t, u, z, a, b, hid, sums, inbox,
                     lsem, wsem, osem, gsend, grecv, xsend, xrecv, ssem):
    ids, core, x, y = place()
    greet(ids)
    load_x = pltpu.make_async_copy(xall_h, xall, lsem.at[0])
    load_x.start()
    weights = Weights((w1_h, w3_h, w2_h), (w1, w3, w2), wsem)
    dy1 = (dy_h[...].astype(F32) + ((r_me[...] + r_x[...]) + (r_y[...] + r_d[...]))).astype(BF16)
    dall[pl.ds(pl.multiple_of(ids["me"] * TOK, TOK), TOK), :] = dy1
    dy1_o[...] = dy1
    await_peers()
    gd = Gather(ids, dall, gsend, grecv, 2)
    gd.start(PRIM)
    load_x.wait()
    weights.start((0, 1), (0, 1))
    build_onehot(table, 16, ids["me"], onehot, gate_col)
    weights.start((0, 1), (2, 3, 4))
    take_rows(onehot, xall, u)
    weights.start((2,), range(LOCAL))
    gd.start(SEC)
    gd.start(PARTNER)
    build_scatter(onehot, scatter)
    store_u = pltpu.make_async_copy(u, u_o, osem.at[0])
    store_u.start()

    def forward(first, last):
        def step(e, carry):
            weights.wait((0, 1), e)
            forward_expert(e, u, w1, w3, a, b, hid)
            return carry
        lax.fori_loop(first, last, step, 0)

    forward(0, 1)
    gd.relay_prim(0)
    forward(1, 2)
    gd.relay_prim(1)
    forward(2, LOCAL)
    gd.relay_rest(0)
    for e in range(LOCAL):
        weights.wait((2,), e)
        turn_wide(w2, w2t, e)
    gd.relay_rest(1)
    gd.finish()
    take_rows(onehot, dall, z, gate_col)
    store_z = pltpu.make_async_copy(z, z_o, osem.at[1])
    store_h = pltpu.make_async_copy(hid, hid_o, osem.at[2])
    store_z.start()
    store_h.start()
    for e in range(LOCAL):
        hidden_grads(e, z, w2t, a, b)
    store_a = pltpu.make_async_copy(a, da_o, osem.at[3])
    store_b = pltpu.make_async_copy(b, db_o, osem.at[4])
    store_a.start()
    store_b.start()
    return_sums(ids, core, x, y, scatter, False, w1, w3, a, b, xall, sums, inbox, xsend, xrecv, ssem, (s_me, s_x, s_y, s_d), lambda n: None)
    gd.drain()
    for c in (store_u, store_z, store_h, store_a, store_b):
        c.wait()


HBM_SPEC = pl.BlockSpec(memory_space=pltpu.HBM)
VMEM_SPEC = pl.BlockSpec(memory_space=pltpu.VMEM)


def compute_scratch():
    return [
        pltpu.VMEM((LOCAL, D, F), BF16), pltpu.VMEM((LOCAL, D, F), BF16), pltpu.VMEM((LOCAL, F, D), BF16),
        pltpu.VMEM((2, SLOTS, 256), BF16), pltpu.VMEM((2, 256, SLOTS), BF16), pltpu.VMEM((2, LOCAL * HALF_ROWS, 128), F32), pltpu.VMEM((LOCAL, D, F), BF16),
        pltpu.VMEM((LOCAL, ROWS, D), BF16), pltpu.VMEM((LOCAL, ROWS, D), BF16),
        pltpu.VMEM((LOCAL, ROWS, F), BF16), pltpu.VMEM((LOCAL, ROWS, F), BF16), pltpu.VMEM((LOCAL, ROWS, F), BF16),
        pltpu.VMEM((8 * TOK, D), F32), pltpu.VMEM((4, TOK, D), F32),
    ]


ROW_OUTS = [jax.ShapeDtypeStruct((LOCAL, ROWS, D), BF16)] * 2 + [jax.ShapeDtypeStruct((LOCAL, ROWS, F), BF16)] * 3
SUM_OUTS = [jax.ShapeDtypeStruct((TOK, D), F32)] * 4
DMA = pltpu.SemaphoreType.DMA


def layer_two(routing, y_mid, dy_out, x_tokens, w1, w3, w2):
    all_tok = pltpu.VMEM((8 * TOK, D), BF16)
    table_in = [pltpu.VMEM((8, TOK), t) for t in (jnp.int32, jnp.int32, F32)]
    return pl.pallas_call(
        layer_two_kernel, name="layer_two",
        out_shape=ROW_OUTS + [jax.ShapeDtypeStruct((8 * TOK, D), BF16), jax.ShapeDtypeStruct((32, 8 * TOK), F32)] + SUM_OUTS,
        in_specs=[HBM_SPEC] * 12, out_specs=[HBM_SPEC] * 11,
        scratch_shapes=table_in * 2 + [pltpu.VMEM((8, 32, 128), F32), all_tok, all_tok, all_tok] + compute_scratch() + [pltpu.VMEM((LOCAL, F, D), BF16), pltpu.VMEM((32, 8 * TOK), F32)]
        + [DMA((9,)), DMA((3, LOCAL)), DMA((7,)), DMA((1,)), DMA((4,)), DMA((3, 1)), DMA((3, 7)), DMA((1,)), DMA((len(CHUNKS),)), DMA((4,))],
        compiler_params=pltpu.CompilerParams(collective_id=0, has_side_effects=True, vmem_limit_bytes=63 * 2**20),
        cost_estimate=pl.CostEstimate(flops=16 * 10**9, bytes_accessed=36 * 2**20, transcendentals=0),
    )(*routing, y_mid, dy_out, x_tokens, w1, w3, w2)


def layer_one(dy_out, returned, table, xall, w1, w3, w2):
    all_tok = pltpu.VMEM((8 * TOK, D), BF16)
    return pl.pallas_call(
        layer_one_kernel, name="layer_one",
        out_shape=ROW_OUTS + [jax.ShapeDtypeStruct((TOK, D), BF16)] + SUM_OUTS,
        in_specs=[VMEM_SPEC] * 6 + [HBM_SPEC] * 4, out_specs=[HBM_SPEC] * 5 + [VMEM_SPEC] + [HBM_SPEC] * 4,
        scratch_shapes=[all_tok, all_tok] + compute_scratch()
        + [DMA((1,)), DMA((3, LOCAL)), DMA((5,)), DMA((1,)), DMA((7,)), DMA((1,)), DMA((len(CHUNKS),)), DMA((4,))],
        compiler_params=pltpu.CompilerParams(collective_id=1, has_side_effects=True, vmem_limit_bytes=50 * 2**20),
        cost_estimate=pl.CostEstimate(flops=16 * 10**9, bytes_accessed=36 * 2**20, transcendentals=0),
    )(dy_out, *returned, table, xall, w1, w3, w2)


PARTS = 4


def weight_grad_kernel(u_h, z_h, hid_h, da_h, db_h, dw1_h, dw3_h, dw2_h, u, z, hid, da, db, ring1, ring3, ring2, isem, osem):
    def load(e):
        return [pltpu.make_async_copy(src.at[e], dst.at[e], isem.at[k, e]) for k, (src, dst) in enumerate(((u_h, u), (da_h, da), (db_h, db), (hid_h, hid), (z_h, z)))]

    for e in range(LOCAL):
        for c in load(e):
            c.start()

    def store(e, p):
        rows, cols = D // PARTS, F // PARTS
        return [pltpu.make_async_copy(ring1.at[p], dw1_h.at[e, pl.ds(p * rows, rows)], osem.at[0, p]),
                pltpu.make_async_copy(ring3.at[p], dw3_h.at[e, pl.ds(p * rows, rows)], osem.at[1, p]),
                pltpu.make_async_copy(ring2.at[p], dw2_h.at[e, pl.ds(p * cols, cols)], osem.at[2, p])]

    def expert(e, carry):
        for c in load(e):
            c.wait()
        for p in range(PARTS):
            rows, cols = slice(p * (D // PARTS), (p + 1) * (D // PARTS)), slice(p * (F // PARTS), (p + 1) * (F // PARTS))
            out = store(e, p)

            @pl.when(e > 0)
            def _():
                for c in out:
                    c.wait()

            ring1[p] = lax.dot_general(u[e, :, rows], da[e], TRANS_A, preferred_element_type=F32)
            out[0].start()
            ring3[p] = lax.dot_general(u[e, :, rows], db[e], TRANS_A, preferred_element_type=F32)
            out[1].start()
            ring2[p] = lax.dot_general(hid[e, :, cols], z[e], TRANS_A, preferred_element_type=F32)
            out[2].start()
        return carry

    lax.fori_loop(0, LOCAL, expert, 0)
    for p in range(PARTS):
        for c in store(LOCAL - 1, p):
            c.wait()


def weight_grads(u, z, hid, da, db):
    wide, narrow = pltpu.VMEM((LOCAL, ROWS, D), BF16), pltpu.VMEM((LOCAL, ROWS, F), BF16)
    ring = pltpu.VMEM((PARTS, D // PARTS, F), F32)
    return pl.pallas_call(
        weight_grad_kernel, name="weight_grads",
        in_specs=[HBM_SPEC] * 5, out_specs=[HBM_SPEC] * 3,
        out_shape=[jax.ShapeDtypeStruct((LOCAL, D, F), F32)] * 2 + [jax.ShapeDtypeStruct((LOCAL, F, D), F32)],
        scratch_shapes=[wide, wide, narrow, narrow, narrow, ring, ring, pltpu.VMEM((PARTS, F // PARTS, D), F32), DMA((5, LOCAL)), DMA((3, PARTS))],
        compiler_params=pltpu.CompilerParams(vmem_limit_bytes=60 * 2**20),
        cost_estimate=pl.CostEstimate(flops=18 * 10**9, bytes_accessed=56 * 2**20, transcendentals=0),
    )(u, z, hid, da, db)


def exchange_sums(sums):
    swap = lambda mask: [(i, i ^ mask) for i in range(8)]
    return (sums[0],) + tuple(lax.ppermute(sums[k], "expert", swap(mask)) for k, mask in ((1, 2), (2, 4), (3, 6)))


def solution(mesh):
    tok_spec = P(("data", "expert"), None)
    weight_spec = P("expert", None, None)
    grad_spec = P(("data", "expert"), None, None)

    def local_step(x_tokens, y_mid, dy_out, experts_one, gates_one, slots_one, experts_two, gates_two, slots_two, w_gate_one, w_up_one, w_down_one, w_gate_two, w_up_two, w_down_two):
        routing = [r.T for r in (experts_two, slots_two, gates_two, experts_one, slots_one, gates_one)]
        *rows_two, xall, table, s0, s1, s2, s3 = layer_two(routing, y_mid, dy_out, x_tokens, w_gate_two, w_up_two, w_down_two)
        returned = exchange_sums((s0, s1, s2, s3))
        grads_two = weight_grads(*rows_two)
        *rows_one, dy_mid, s0, s1, s2, s3 = layer_one(dy_out, returned, table, xall, w_gate_one, w_up_one, w_down_one)
        r = exchange_sums((s0, s1, s2, s3))
        grads_one = weight_grads(*rows_one)
        dx_tokens = (dy_mid.astype(F32) + ((r[0] + r[1]) + (r[2] + r[3]))).astype(BF16)
        return (dx_tokens, *grads_one, *grads_two)

    return jax.shard_map(local_step, mesh=mesh, in_specs=(tok_spec,) * 9 + (weight_spec,) * 6, out_specs=(tok_spec,) + (grad_spec,) * 6, check_vma=False)
```

```python
import functools
import jax
import jax.numpy as jnp
from jax import lax
from jax.experimental import pallas as pl
from jax.experimental.pallas import tpu as pltpu
from jax.sharding import PartitionSpec as P

MESH = pl.DeviceIdType.MESH
F32 = jnp.float32
BF16 = jnp.bfloat16
CAP = 24
LOCAL = 5
D = 1536
F = 512
TOK = 64
HALF_ROWS = 4 * CAP
ROWS = 8 * CAP
STEP = 512
SLOTS = 512
CHUNKS = ((0, 768), (768, 512), (1280, 256))


def place():
    me = lax.axis_index("expert")
    core, x, y = me % 2, (me // 2) % 2, me // 4
    ident = lambda xx, yy, cc: 4 * yy + 2 * xx + cc
    ids = {
        "me": me,
        "partner": ident(x, y, 1 - core),
        "x": ident(1 - x, y, core),
        "y": ident(x, 1 - y, core),
        "diag": ident(1 - x, 1 - y, core),
        "prim": ident(x + (1 - core) * (1 - 2 * x), y + core * (1 - 2 * y), core),
        "sec": ident(x + core * (1 - 2 * x), y + (1 - core) * (1 - 2 * y), core),
        "p_prim": ident(x + core * (1 - 2 * x), y + (1 - core) * (1 - 2 * y), 1 - core),
        "p_sec": ident(x + (1 - core) * (1 - 2 * x), y + core * (1 - 2 * y), 1 - core),
        "p_diag": ident(1 - x, 1 - y, 1 - core),
    }
    return ids, core, x, y


def greet(ids):
    for peer in ("partner", "x", "y"):
        pl.semaphore_signal(pltpu.get_barrier_semaphore(), inc=1, device_id={"expert": ids[peer]}, device_id_type=MESH)


def await_peers():
    pl.semaphore_wait(pltpu.get_barrier_semaphore(), 3)


def block(ref, ident):
    return ref.at[pl.ds(pl.multiple_of(ident * TOK, TOK), TOK)]


class Gather:
    ROUTES = (("me", "partner"), ("me", "prim"), ("me", "sec"), ("prim", "sec"), ("prim", "partner"), ("sec", "partner"), ("diag", "partner"))
    ARRIVE = ("partner", "prim", "sec", "diag", "p_prim", "p_sec", "p_diag")

    def __init__(self, ids, ref, send, recv, pieces):
        self.ids, self.ref, self.send, self.recv, self.pieces = ids, ref, send, recv, pieces

    def part(self, ident, i):
        if self.pieces == 0:
            return self.ref.at[ident]
        size = TOK // self.pieces
        return self.ref.at[pl.ds(pl.multiple_of(ident * TOK + i * size, size), size)]

    def arrival(self, k, i):
        return self.recv.at[3 * i + k - 1] if 1 <= k <= 3 else self.recv.at[3 * max(self.pieces, 1)]

    def copy(self, k, i, what=None, where=None):
        what, where = what or self.ROUTES[k][0], where or self.ROUTES[k][1]
        part = self.part(self.ids[what], i)
        return pltpu.make_async_remote_copy(src_ref=part, dst_ref=part, send_sem=self.send.at[0], recv_sem=self.arrival(k, i), device_id={"expert": self.ids[where]}, device_id_type=MESH)

    def arrived(self, k, i):
        self.copy(k, i, self.ARRIVE[k], "partner").wait_recv()

    def every(self):
        return range(max(self.pieces, 1))

    def start(self, k):
        for i in self.every():
            self.copy(k, i).start()

    def relay_prim(self, i):
        self.arrived(1, i)
        self.copy(3, i).start()
        self.copy(4, i).start()

    def relay_rest(self, i):
        self.arrived(2, i)
        self.copy(5, i).start()
        self.arrived(3, i)
        self.copy(6, i).start()

    def blocks(self, count):
        part = self.ref.at[pl.ds(0, count * (TOK if self.pieces else 1))]
        return pltpu.make_async_remote_copy(src_ref=part, dst_ref=part, send_sem=self.send.at[0], recv_sem=self.recv.at[3 * max(self.pieces, 1)], device_id={"expert": self.ids["partner"]}, device_id_type=MESH)

    def finish(self):
        self.blocks(4).wait_recv()

    def drain(self):
        self.blocks(7).wait_send()


PARTNER, PRIM, SEC = 0, 1, 2


def fill_table(routing, me, out):
    out[...] = jnp.zeros((32, 128), F32)
    for layer in range(2):
        experts, slots, gates = (routing[3 * layer + k] for k in range(3))
        keys = jnp.where(slots[...] >= 0, experts[...] * HALF_ROWS + (me % 4) * CAP + slots[...], -1)
        out[16 * layer : 16 * layer + 8, 0:TOK] = keys.astype(F32)
        out[16 * layer + 8 : 16 * layer + 16, 0:TOK] = gates[...]


def join_table(tab, table):
    low = lax.broadcasted_iota(jnp.int32, (32, 128), 1) < TOK
    for p in range(4):
        table[:, p * 128 : (p + 1) * 128] = jnp.where(low, tab[2 * p], pltpu.roll(tab[2 * p + 1], TOK, 1))


def build_onehot(table, base, me, onehot, gate_col):
    for h in range(2):
        onehot[h, LOCAL * HALF_ROWS : SLOTS, :] = jnp.zeros((SLOTS - LOCAL * HALF_ROWS, 256), BF16)
        cols = slice(h * 256, (h + 1) * 256)
        keys = [table[base + j : base + j + 1, cols] for j in range(8)]
        gates = [table[base + 8 + j : base + 9 + j, cols] for j in range(8)]
        for e in range(LOCAL):
            row = (lax.broadcasted_iota(jnp.int32, (HALF_ROWS, 256), 0) + (e + me * LOCAL) * HALF_ROWS).astype(F32)
            gate = jnp.zeros((HALF_ROWS, 256), F32)
            hit = jnp.zeros((HALF_ROWS, 256), F32)
            for j in range(8):
                match = row == keys[j]
                gate = jnp.where(match, gates[j], gate)
                hit = jnp.where(match, 1.0, hit)
            onehot[h, e * HALF_ROWS : (e + 1) * HALF_ROWS, :] = hit.astype(BF16)
            gate_col[h, e * HALF_ROWS : (e + 1) * HALF_ROWS, :] = jnp.broadcast_to(jnp.sum(gate, axis=1, keepdims=True), (HALF_ROWS, 128))


def build_scatter(onehot, scatter):
    for h in range(2):
        scatter[h] = jnp.transpose(onehot[h])


def turn_tall(src, dst, e):
    for n in range(D // 128):
        dst[e, :, n * 128 : (n + 1) * 128] = jnp.transpose(src[e, n * 128 : (n + 1) * 128, :])


def turn_wide(src, dst, e):
    for n in range(D // 128):
        dst[e, n * 128 : (n + 1) * 128, :] = jnp.transpose(src[e, :, n * 128 : (n + 1) * 128])


def take_rows(onehot, tokens, rows, gate_col=None):
    for h in range(2):
        for n in range(D // STEP):
            cols = slice(n * STEP, (n + 1) * STEP)
            out = jnp.dot(onehot[h, 0 : LOCAL * HALF_ROWS], tokens[h * 256 : (h + 1) * 256, cols], preferred_element_type=F32)
            if gate_col is not None:
                out = out * gate_col[h, :, 0:1]
            out = out.astype(BF16)
            for e in range(LOCAL):
                rows[e, h * HALF_ROWS : (h + 1) * HALF_ROWS, cols] = out[e * HALF_ROWS : (e + 1) * HALF_ROWS]


def forward_expert(e, u, w1, w3, a, b, hid):
    act = jnp.dot(u[e], w1[e], preferred_element_type=F32).astype(BF16)
    up = jnp.dot(u[e], w3[e], preferred_element_type=F32).astype(BF16)
    a[e] = act
    b[e] = up
    wide = act.astype(F32)
    hid[e] = (wide * jax.nn.sigmoid(wide) * up.astype(F32)).astype(BF16)


TRANS_B = (((1,), (1,)), ((), ()))
TRANS_A = (((0,), (0,)), ((), ()))


def hidden_grads(e, z, w2, a, b):
    dh = jnp.dot(z[e], w2[e], preferred_element_type=F32)
    act = a[e].astype(F32)
    up = b[e].astype(F32)
    sig = jax.nn.sigmoid(act)
    a[e] = (dh * up * sig * (1.0 + act * (1.0 - sig))).astype(BF16)
    b[e] = (dh * (act * sig)).astype(BF16)


def row_grads(e, cols, turned, w1, w3, a, b, dxr):
    dx = jnp.dot(a[e], w1[e, :, cols], preferred_element_type=F32)
    if turned:
        dx = dx + jnp.dot(b[e], w3[e, :, cols], preferred_element_type=F32)
    else:
        dx = dx + lax.dot_general(b[e], w3[e, cols, :], TRANS_B, preferred_element_type=F32)
    dx = dx.astype(BF16)
    for h in range(2):
        dxr[e * HALF_ROWS : (e + 1) * HALF_ROWS, h * (D // 2) : h * (D // 2) + dx.shape[1]] = dx[h * HALF_ROWS : (h + 1) * HALF_ROWS]


def return_sums(ids, core, x, y, scatter, turned, w1, w3, a, b, dxr, sums, inbox, send, recv, ssem, outs, between):
    def exchange(n, yy, xx):
        theirs = 4 * yy + 2 * xx + (1 - core)
        cols = pl.ds(*CHUNKS[n])
        src = sums.at[pl.ds(pl.multiple_of(theirs * TOK, TOK), TOK), cols]
        return pltpu.make_async_remote_copy(src_ref=src, dst_ref=inbox.at[2 * yy + xx, :, cols], send_sem=send.at[0], recv_sem=recv.at[n], device_id={"expert": ids["partner"]}, device_id_type=MESH)

    def whole(ref, sem):
        return pltpu.make_async_remote_copy(src_ref=ref, dst_ref=ref, send_sem=send.at[0], recv_sem=sem, device_id={"expert": ids["partner"]}, device_id_type=MESH)

    def store(n, name, xx, yy, out, k):
        cols = pl.ds(*CHUNKS[n])
        return pltpu.make_async_copy(inbox.at[2 * yy + xx, :, cols], out.at[:, cols], ssem.at[k])

    blocks = (("me", x, y, outs[0], 0), ("x", 1 - x, y, outs[1], 1), ("y", x, 1 - y, outs[2], 2), ("diag", 1 - x, 1 - y, outs[3], 3))

    def collect(n):
        cols = slice(CHUNKS[n][0], sum(CHUNKS[n]))
        whole(inbox.at[:, :, cols], recv.at[n]).wait_recv()
        for name, xx, yy, out, k in blocks:
            inbox[2 * yy + xx, :, cols] = inbox[2 * yy + xx, :, cols] + sums[pl.ds(pl.multiple_of(ids[name] * TOK, TOK), TOK), cols]
            store(n, name, xx, yy, out, k).start()

    for n in range(len(CHUNKS)):
        cols = slice(CHUNKS[n][0], sum(CHUNKS[n]))
        for e in range(LOCAL):
            row_grads(e, cols, turned, w1, w3, a, b, dxr)
        for h in range(2):
            sums[h * 256 : (h + 1) * 256, cols] = jnp.dot(scatter[h, :, 0 : LOCAL * HALF_ROWS], dxr[0 : LOCAL * HALF_ROWS, h * (D // 2) : h * (D // 2) + CHUNKS[n][1]], preferred_element_type=F32)
        for k in range(4):
            exchange(n, k // 2, k % 2).start()
        if n == 2:
            collect(0)
        between(n)
    collect(1)
    collect(2)
    whole(inbox, recv.at[0]).wait_send()
    for name, xx, yy, out, k in blocks:
        pltpu.make_async_copy(inbox.at[2 * yy + xx], out, ssem.at[k]).wait()


class Weights:
    def __init__(self, hbm, vmem, sems):
        self.hbm, self.vmem, self.sems = hbm, vmem, sems

    def copy(self, k, e):
        return pltpu.make_async_copy(self.hbm[k].at[e], self.vmem[k].at[e], self.sems.at[k, e])

    def start(self, kinds, experts):
        for e in experts:
            for k in kinds:
                self.copy(k, e).start()

    def wait(self, kinds, e):
        for k in kinds:
            self.copy(k, e).wait()


def layer_two_kernel(*refs):
    routing_h, refs = refs[:6], refs[6:]
    (y_h, dy_h, x_h, w1_h, w3_h, w2_h,
     u_o, z_o, hid_o, da_o, db_o, xall_o, table_o, s_me, s_x, s_y, s_d) = refs[:17]
    routing, refs = refs[17:23], refs[23:]
    (tab, yall, dall, xall, w1, w3, w2, onehot, scatter, gate_col, w2t, u, z, a, b, hid, sums, inbox, w3t, table,
     lsem, wsem, osem, tsend, trecv, gsend, grecv, xsend, xrecv, ssem) = refs
    ids, core, x, y = place()
    greet(ids)
    small = [pltpu.make_async_copy(src, dst, lsem.at[3 + i]) for i, (src, dst) in enumerate(zip(routing_h, routing))]
    local = [pltpu.make_async_copy(src, block(dst, ids["me"]), lsem.at[i]) for i, (src, dst) in enumerate(((y_h, yall), (dy_h, dall), (x_h, xall)))]
    for c in small + local:
        c.start()
    for c in small:
        c.wait()
    fill_table(routing, ids["me"], tab.at[ids["me"]])
    local[0].wait()
    weights = Weights((w1_h, w3_h, w2_h), (w1, w3, w2), wsem)
    gt = Gather(ids, tab, tsend, trecv, 0)
    gy, gd, gx = [Gather(ids, ref, gsend.at[i], grecv.at[i], 2) for i, ref in enumerate((yall, dall, xall))]
    await_peers()
    gt.start(PRIM)
    gt.start(SEC)
    gy.start(PRIM)
    gt.start(PARTNER)
    for c in local[1:]:
        c.wait()
    weights.start((2,), range(LOCAL))
    weights.start((0, 1), range(LOCAL))

    def turn(first, last):
        for i in range(first, last):
            e = i % LOCAL
            if i < 2 * LOCAL:
                weights.wait(((2,), (0,))[i // LOCAL], e)
            (turn_wide, turn_tall, turn_tall)[i // LOCAL]((w2, w1, w3)[i // LOCAL], (w2t, w2, w3t)[i // LOCAL], e)

    turn(0, 1)
    gy.start(PARTNER)
    turn(1, 2)
    gy.start(SEC)
    turn(2, 3)
    gt.relay_prim(0)
    gy.relay_prim(0)
    turn(3, 5)
    gy.relay_prim(1)
    turn(5, 8)
    gd.start(PRIM)
    gt.relay_rest(0)
    turn(8, 9)
    gt.finish()
    join_table(tab, table)
    save_table = pltpu.make_async_copy(table, table_o, osem.at[6])
    save_table.start()
    build_onehot(table, 0, ids["me"], onehot, gate_col)
    gd.start(SEC)
    gd.start(PARTNER)
    gy.relay_rest(0)
    build_scatter(onehot, scatter)
    for e in range(LOCAL):
        weights.wait((1,), e)
    turn(9, 12)
    gy.relay_rest(1)
    turn(12, 13)
    gy.finish()
    gd.relay_prim(0)
    take_rows(onehot, yall, u)
    store_u = pltpu.make_async_copy(u, u_o, osem.at[0])
    store_u.start()

    def forward(first, last):
        lax.fori_loop(first, last, lambda e, carry: (forward_expert(e, u, w1, w3, a, b, hid), carry)[1], 0)

    gd.relay_prim(1)
    forward(0, 2)
    gx.start(PRIM)
    forward(2, 4)
    gx.start(SEC)
    gd.relay_rest(0)
    forward(4, LOCAL)
    gd.relay_rest(1)
    turn(13, 3 * LOCAL)
    gd.finish()
    gx.start(PARTNER)
    take_rows(onehot, dall, z, gate_col)
    store_z = pltpu.make_async_copy(z, z_o, osem.at[1])
    store_h = pltpu.make_async_copy(hid, hid_o, osem.at[2])
    store_z.start()
    store_h.start()
    gx.relay_prim(0)
    for e in range(LOCAL):
        hidden_grads(e, z, w2t, a, b)
    gx.relay_prim(1)
    store_a = pltpu.make_async_copy(a, da_o, osem.at[3])
    store_b = pltpu.make_async_copy(b, db_o, osem.at[4])
    store_a.start()
    store_b.start()
    store_x = pltpu.make_async_copy(xall, xall_o, osem.at[5])

    def between(n):
        if n == 1:
            gx.relay_rest(0)
            gx.relay_rest(1)
        if n == 2:
            gx.finish()
            store_x.start()

    gy.drain()
    return_sums(ids, core, x, y, scatter, True, w2, w3t, a, b, yall, sums, inbox, xsend, xrecv, ssem, (s_me, s_x, s_y, s_d), between)
    for g in (gt, gd, gx):
        g.drain()
    for c in (store_u, store_z, store_h, store_a, store_b, store_x, save_table):
        c.wait()


def layer_one_kernel(dy_h, r_me, r_x, r_y, r_d, table, xall_h, w1_h, w3_h, w2_h,
                     u_o, z_o, hid_o, da_o, db_o, dy1_o, s_me, s_x, s_y, s_d,
                     dall, xall, w1, w3, w2, onehot, scatter, gate_col, w2t, u, z, a, b, hid, sums, inbox,
                     lsem, wsem, osem, gsend, grecv, xsend, xrecv, ssem):
    ids, core, x, y = place()
    greet(ids)
    load_x = pltpu.make_async_copy(xall_h, xall, lsem.at[0])
    load_x.start()
    weights = Weights((w1_h, w3_h, w2_h), (w1, w3, w2), wsem)
    weights.start((0, 1), (0,))
    dy1 = (dy_h[...].astype(F32) + ((r_me[...] + r_x[...]) + (r_y[...] + r_d[...]))).astype(BF16)
    dall[pl.ds(pl.multiple_of(ids["me"] * TOK, TOK), TOK), :] = dy1
    dy1_o[...] = dy1
    await_peers()
    gd = Gather(ids, dall, gsend, grecv, 2)
    gd.start(PRIM)
    build_onehot(table, 16, ids["me"], onehot, gate_col)
    load_x.wait()
    weights.start((0, 1), (1,))
    weights.start((2,), (0, 1, 2))
    weights.start((0, 1), (2, 3, 4))
    weights.start((2,), (3, 4))
    take_rows(onehot, xall, u)
    gd.start(SEC)
    gd.start(PARTNER)
    build_scatter(onehot, scatter)
    store_u = pltpu.make_async_copy(u, u_o, osem.at[0])
    store_u.start()

    def forward(first, last):
        def step(e, carry):
            weights.wait((0, 1), e)
            forward_expert(e, u, w1, w3, a, b, hid)
            return carry
        lax.fori_loop(first, last, step, 0)

    def turn(first, last):
        for i in range(first, last):
            e = i % LOCAL
            if i < LOCAL:
                weights.wait((2,), e)
                turn_wide(w2, w2t, e)
            else:
                turn_tall(w1, w2, e)

    forward(0, 1)
    gd.relay_prim(0)
    forward(1, 2)
    turn(0, 2)
    gd.relay_prim(1)
    turn(2, 3)
    forward(2, LOCAL)
    turn(3, 5)
    gd.relay_rest(0)
    turn(5, 7)
    gd.relay_rest(1)
    turn(7, 2 * LOCAL)
    gd.finish()
    take_rows(onehot, dall, z, gate_col)
    store_z = pltpu.make_async_copy(z, z_o, osem.at[1])
    store_h = pltpu.make_async_copy(hid, hid_o, osem.at[2])
    store_z.start()
    store_h.start()
    for e in range(LOCAL):
        hidden_grads(e, z, w2t, a, b)
    store_a = pltpu.make_async_copy(a, da_o, osem.at[3])
    store_b = pltpu.make_async_copy(b, db_o, osem.at[4])
    store_a.start()
    store_b.start()
    return_sums(ids, core, x, y, scatter, False, w2, w3, a, b, xall, sums, inbox, xsend, xrecv, ssem, (s_me, s_x, s_y, s_d), lambda n: None)
    gd.drain()
    for c in (store_u, store_z, store_h, store_a, store_b):
        c.wait()


HBM_SPEC = pl.BlockSpec(memory_space=pltpu.HBM)
VMEM_SPEC = pl.BlockSpec(memory_space=pltpu.VMEM)


def compute_scratch():
    return [
        pltpu.VMEM((LOCAL, D, F), BF16), pltpu.VMEM((LOCAL, D, F), BF16), pltpu.VMEM((LOCAL, F, D), BF16),
        pltpu.VMEM((2, SLOTS, 256), BF16), pltpu.VMEM((2, 256, SLOTS), BF16), pltpu.VMEM((2, LOCAL * HALF_ROWS, 128), F32), pltpu.VMEM((LOCAL, D, F), BF16),
        pltpu.VMEM((LOCAL, ROWS, D), BF16), pltpu.VMEM((LOCAL, ROWS, D), BF16),
        pltpu.VMEM((LOCAL, ROWS, F), BF16), pltpu.VMEM((LOCAL, ROWS, F), BF16), pltpu.VMEM((LOCAL, ROWS, F), BF16),
        pltpu.VMEM((8 * TOK, D), F32), pltpu.VMEM((4, TOK, D), F32),
    ]


ROW_OUTS = [jax.ShapeDtypeStruct((LOCAL, ROWS, D), BF16)] * 2 + [jax.ShapeDtypeStruct((LOCAL, ROWS, F), BF16)] * 3
SUM_OUTS = [jax.ShapeDtypeStruct((TOK, D), F32)] * 4
DMA = pltpu.SemaphoreType.DMA


def layer_two(routing, y_mid, dy_out, x_tokens, w1, w3, w2):
    all_tok = pltpu.VMEM((8 * TOK, D), BF16)
    table_in = [pltpu.VMEM((8, TOK), t) for t in (jnp.int32, jnp.int32, F32)]
    return pl.pallas_call(
        layer_two_kernel, name="layer_two",
        out_shape=ROW_OUTS + [jax.ShapeDtypeStruct((8 * TOK, D), BF16), jax.ShapeDtypeStruct((32, 8 * TOK), F32)] + SUM_OUTS,
        in_specs=[HBM_SPEC] * 12, out_specs=[HBM_SPEC] * 11,
        scratch_shapes=table_in * 2 + [pltpu.VMEM((8, 32, 128), F32), all_tok, all_tok, all_tok] + compute_scratch() + [pltpu.VMEM((LOCAL, F, D), BF16), pltpu.VMEM((32, 8 * TOK), F32)]
        + [DMA((9,)), DMA((3, LOCAL)), DMA((7,)), DMA((1,)), DMA((4,)), DMA((3, 1)), DMA((3, 7)), DMA((1,)), DMA((len(CHUNKS),)), DMA((4,))],
        compiler_params=pltpu.CompilerParams(collective_id=0, has_side_effects=True, vmem_limit_bytes=63 * 2**20),
        cost_estimate=pl.CostEstimate(flops=16 * 10**9, bytes_accessed=36 * 2**20, transcendentals=0),
    )(*routing, y_mid, dy_out, x_tokens, w1, w3, w2)


def layer_one(dy_out, returned, table, xall, w1, w3, w2):
    all_tok = pltpu.VMEM((8 * TOK, D), BF16)
    return pl.pallas_call(
        layer_one_kernel, name="layer_one",
        out_shape=ROW_OUTS + [jax.ShapeDtypeStruct((TOK, D), BF16)] + SUM_OUTS,
        in_specs=[VMEM_SPEC] * 6 + [HBM_SPEC] * 4, out_specs=[HBM_SPEC] * 5 + [VMEM_SPEC] + [HBM_SPEC] * 4,
        scratch_shapes=[all_tok, all_tok] + compute_scratch()
        + [DMA((1,)), DMA((3, LOCAL)), DMA((5,)), DMA((1,)), DMA((7,)), DMA((1,)), DMA((len(CHUNKS),)), DMA((4,))],
        compiler_params=pltpu.CompilerParams(collective_id=1, has_side_effects=True, vmem_limit_bytes=50 * 2**20),
        cost_estimate=pl.CostEstimate(flops=16 * 10**9, bytes_accessed=36 * 2**20, transcendentals=0),
    )(dy_out, *returned, table, xall, w1, w3, w2)


PARTS = 4


def weight_grad_kernel(u_h, z_h, hid_h, da_h, db_h, dw1_h, dw3_h, dw2_h, u, z, hid, da, db, ring1, ring3, ring2, isem, osem):
    def load(e):
        return [pltpu.make_async_copy(src.at[e], dst.at[e], isem.at[k, e]) for k, (src, dst) in enumerate(((u_h, u), (da_h, da), (db_h, db), (hid_h, hid), (z_h, z)))]

    for e in range(LOCAL):
        for c in load(e):
            c.start()

    def store(e, p):
        rows, cols = D // PARTS, F // PARTS
        return [pltpu.make_async_copy(ring1.at[p], dw1_h.at[e, pl.ds(p * rows, rows)], osem.at[0, p]),
                pltpu.make_async_copy(ring3.at[p], dw3_h.at[e, pl.ds(p * rows, rows)], osem.at[1, p]),
                pltpu.make_async_copy(ring2.at[p], dw2_h.at[e, pl.ds(p * cols, cols)], osem.at[2, p])]

    def expert(e, carry):
        for c in load(e):
            c.wait()
        for p in range(PARTS):
            rows, cols = slice(p * (D // PARTS), (p + 1) * (D // PARTS)), slice(p * (F // PARTS), (p + 1) * (F // PARTS))
            out = store(e, p)

            @pl.when(e > 0)
            def _():
                for c in out:
                    c.wait()

            ring1[p] = lax.dot_general(u[e, :, rows], da[e], TRANS_A, preferred_element_type=F32)
            out[0].start()
            ring3[p] = lax.dot_general(u[e, :, rows], db[e], TRANS_A, preferred_element_type=F32)
            out[1].start()
            ring2[p] = lax.dot_general(hid[e, :, cols], z[e], TRANS_A, preferred_element_type=F32)
            out[2].start()
        return carry

    lax.fori_loop(0, LOCAL, expert, 0)
    for p in range(PARTS):
        for c in store(LOCAL - 1, p):
            c.wait()


def weight_grads(u, z, hid, da, db):
    wide, narrow = pltpu.VMEM((LOCAL, ROWS, D), BF16), pltpu.VMEM((LOCAL, ROWS, F), BF16)
    ring = pltpu.VMEM((PARTS, D // PARTS, F), F32)
    return pl.pallas_call(
        weight_grad_kernel, name="weight_grads",
        in_specs=[HBM_SPEC] * 5, out_specs=[HBM_SPEC] * 3,
        out_shape=[jax.ShapeDtypeStruct((LOCAL, D, F), F32)] * 2 + [jax.ShapeDtypeStruct((LOCAL, F, D), F32)],
        scratch_shapes=[wide, wide, narrow, narrow, narrow, ring, ring, pltpu.VMEM((PARTS, F // PARTS, D), F32), DMA((5, LOCAL)), DMA((3, PARTS))],
        compiler_params=pltpu.CompilerParams(vmem_limit_bytes=60 * 2**20),
        cost_estimate=pl.CostEstimate(flops=18 * 10**9, bytes_accessed=56 * 2**20, transcendentals=0),
    )(u, z, hid, da, db)


def exchange_sums(sums):
    swap = lambda mask: [(i, i ^ mask) for i in range(8)]
    return (sums[0],) + tuple(lax.ppermute(sums[k], "expert", swap(mask)) for k, mask in ((1, 2), (2, 4), (3, 6)))


def solution(mesh):
    tok_spec = P(("data", "expert"), None)
    weight_spec = P("expert", None, None)
    grad_spec = P(("data", "expert"), None, None)

    def local_step(x_tokens, y_mid, dy_out, experts_one, gates_one, slots_one, experts_two, gates_two, slots_two, w_gate_one, w_up_one, w_down_one, w_gate_two, w_up_two, w_down_two):
        routing = [r.T for r in (experts_two, slots_two, gates_two, experts_one, slots_one, gates_one)]
        *rows_two, xall, table, s0, s1, s2, s3 = layer_two(routing, y_mid, dy_out, x_tokens, w_gate_two, w_up_two, w_down_two)
        returned = exchange_sums((s0, s1, s2, s3))
        grads_two = weight_grads(*rows_two)
        *rows_one, dy_mid, s0, s1, s2, s3 = layer_one(dy_out, returned, table, xall, w_gate_one, w_up_one, w_down_one)
        r = exchange_sums((s0, s1, s2, s3))
        grads_one = weight_grads(*rows_one)
        dx_tokens = (dy_mid.astype(F32) + ((r[0] + r[1]) + (r[2] + r[3]))).astype(BF16)
        return (dx_tokens, *grads_one, *grads_two)

    return jax.shard_map(local_step, mesh=mesh, in_specs=(tok_spec,) * 9 + (weight_spec,) * 6, out_specs=(tok_spec,) + (grad_spec,) * 6, check_vma=False)
```

```python
import functools
import jax
import jax.numpy as jnp
from jax import lax
from jax.experimental import pallas as pl
from jax.experimental.pallas import tpu as pltpu
from jax.sharding import PartitionSpec as P

MESH = pl.DeviceIdType.MESH
F32 = jnp.float32
BF16 = jnp.bfloat16
CAP = 24
LOCAL = 5
D = 1536
F = 512
TOK = 64
HALF_ROWS = 4 * CAP
ROWS = 8 * CAP
STEP = 512
SLOTS = 512
TURNED = 5
CHUNKS = ((0, 768), (768, 512), (1280, 256))


def place():
    me = lax.axis_index("expert")
    core, x, y = me % 2, (me // 2) % 2, me // 4
    ident = lambda xx, yy, cc: 4 * yy + 2 * xx + cc
    ids = {
        "me": me,
        "partner": ident(x, y, 1 - core),
        "x": ident(1 - x, y, core),
        "y": ident(x, 1 - y, core),
        "diag": ident(1 - x, 1 - y, core),
        "prim": ident(x + (1 - core) * (1 - 2 * x), y + core * (1 - 2 * y), core),
        "sec": ident(x + core * (1 - 2 * x), y + (1 - core) * (1 - 2 * y), core),
        "p_prim": ident(x + core * (1 - 2 * x), y + (1 - core) * (1 - 2 * y), 1 - core),
        "p_sec": ident(x + (1 - core) * (1 - 2 * x), y + core * (1 - 2 * y), 1 - core),
        "p_diag": ident(1 - x, 1 - y, 1 - core),
    }
    return ids, core, x, y


def greet(ids):
    for peer in ("partner", "x", "y"):
        pl.semaphore_signal(pltpu.get_barrier_semaphore(), inc=1, device_id={"expert": ids[peer]}, device_id_type=MESH)


def await_peers():
    pl.semaphore_wait(pltpu.get_barrier_semaphore(), 3)


def block(ref, ident):
    return ref.at[pl.ds(pl.multiple_of(ident * TOK, TOK), TOK)]


class Gather:
    ROUTES = (("me", "partner"), ("me", "prim"), ("me", "sec"), ("prim", "sec"), ("prim", "partner"), ("sec", "partner"), ("diag", "partner"))
    ARRIVE = ("partner", "prim", "sec", "diag", "p_prim", "p_sec", "p_diag")

    def __init__(self, ids, ref, send, recv, pieces):
        self.ids, self.ref, self.send, self.recv, self.pieces = ids, ref, send, recv, pieces

    def part(self, ident, i):
        if self.pieces == 0:
            return self.ref.at[ident]
        size = TOK // self.pieces
        return self.ref.at[pl.ds(pl.multiple_of(ident * TOK + i * size, size), size)]

    def arrival(self, k, i):
        return self.recv.at[3 * i + k - 1] if 1 <= k <= 3 else self.recv.at[3 * max(self.pieces, 1)]

    def copy(self, k, i, what=None, where=None):
        what, where = what or self.ROUTES[k][0], where or self.ROUTES[k][1]
        part = self.part(self.ids[what], i)
        return pltpu.make_async_remote_copy(src_ref=part, dst_ref=part, send_sem=self.send.at[0], recv_sem=self.arrival(k, i), device_id={"expert": self.ids[where]}, device_id_type=MESH)

    def arrived(self, k, i):
        self.copy(k, i, self.ARRIVE[k], "partner").wait_recv()

    def every(self):
        return range(max(self.pieces, 1))

    def start(self, k):
        for i in self.every():
            self.copy(k, i).start()

    def relay_prim(self, i):
        self.arrived(1, i)
        self.copy(3, i).start()
        self.copy(4, i).start()

    def relay_rest(self, i):
        self.arrived(2, i)
        self.copy(5, i).start()
        self.arrived(3, i)
        self.copy(6, i).start()

    def blocks(self, count):
        part = self.ref.at[pl.ds(0, count * (TOK if self.pieces else 1))]
        return pltpu.make_async_remote_copy(src_ref=part, dst_ref=part, send_sem=self.send.at[0], recv_sem=self.recv.at[3 * max(self.pieces, 1)], device_id={"expert": self.ids["partner"]}, device_id_type=MESH)

    def finish(self):
        self.blocks(4).wait_recv()

    def drain(self):
        self.blocks(7).wait_send()


PARTNER, PRIM, SEC = 0, 1, 2


def fill_table(routing, me, out):
    out[...] = jnp.zeros((32, 128), F32)
    for layer in range(2):
        experts, slots, gates = (routing[3 * layer + k] for k in range(3))
        keys = jnp.where(slots[...] >= 0, experts[...] * HALF_ROWS + (me % 4) * CAP + slots[...], -1)
        out[16 * layer : 16 * layer + 8, 0:TOK] = keys.astype(F32)
        out[16 * layer + 8 : 16 * layer + 16, 0:TOK] = gates[...]


def join_table(tab, table):
    low = lax.broadcasted_iota(jnp.int32, (32, 128), 1) < TOK
    for p in range(4):
        table[:, p * 128 : (p + 1) * 128] = jnp.where(low, tab[2 * p], pltpu.roll(tab[2 * p + 1], TOK, 1))


def build_onehot(table, base, me, onehot, gate_col):
    for h in range(2):
        onehot[h, LOCAL * HALF_ROWS : SLOTS, :] = jnp.zeros((SLOTS - LOCAL * HALF_ROWS, 256), BF16)
        cols = slice(h * 256, (h + 1) * 256)
        keys = [table[base + j : base + j + 1, cols] for j in range(8)]
        gates = [table[base + 8 + j : base + 9 + j, cols] for j in range(8)]
        for e in range(LOCAL):
            row = (lax.broadcasted_iota(jnp.int32, (HALF_ROWS, 256), 0) + (e + me * LOCAL) * HALF_ROWS).astype(F32)
            gate = jnp.zeros((HALF_ROWS, 256), F32)
            hit = jnp.zeros((HALF_ROWS, 256), F32)
            for j in range(8):
                match = row == keys[j]
                gate = jnp.where(match, gates[j], gate)
                hit = jnp.where(match, 1.0, hit)
            onehot[h, e * HALF_ROWS : (e + 1) * HALF_ROWS, :] = hit.astype(BF16)
            gate_col[h, e * HALF_ROWS : (e + 1) * HALF_ROWS, :] = jnp.broadcast_to(jnp.sum(gate, axis=1, keepdims=True), (HALF_ROWS, 128))


def build_scatter(onehot, scatter):
    for h in range(2):
        scatter[h] = jnp.transpose(onehot[h])


def turn_tall(src, dst, e):
    for n in range(D // 128):
        dst[e, :, n * 128 : (n + 1) * 128] = jnp.transpose(src[e, n * 128 : (n + 1) * 128, :])


def turn_wide(src, dst, e):
    for n in range(D // 128):
        dst[e, n * 128 : (n + 1) * 128, :] = jnp.transpose(src[e, :, n * 128 : (n + 1) * 128])


def take_rows(onehot, tokens, rows, gate_col=None):
    for h in range(2):
        for n in range(D // STEP):
            cols = slice(n * STEP, (n + 1) * STEP)
            out = jnp.dot(onehot[h, 0 : LOCAL * HALF_ROWS], tokens[h * 256 : (h + 1) * 256, cols], preferred_element_type=F32)
            if gate_col is not None:
                out = out * gate_col[h, :, 0:1]
            out = out.astype(BF16)
            for e in range(LOCAL):
                rows[e, h * HALF_ROWS : (h + 1) * HALF_ROWS, cols] = out[e * HALF_ROWS : (e + 1) * HALF_ROWS]


def forward_expert(e, u, w1, w3, a, b, hid):
    act = jnp.dot(u[e], w1[e], preferred_element_type=F32).astype(BF16)
    up = jnp.dot(u[e], w3[e], preferred_element_type=F32).astype(BF16)
    a[e] = act
    b[e] = up
    wide = act.astype(F32)
    hid[e] = (wide * jax.nn.sigmoid(wide) * up.astype(F32)).astype(BF16)


TRANS_B = (((1,), (1,)), ((), ()))
TRANS_A = (((0,), (0,)), ((), ()))


def hidden_grads(e, z, w2, a, b):
    dh = jnp.dot(z[e], w2[e], preferred_element_type=F32)
    act = a[e].astype(F32)
    up = b[e].astype(F32)
    sig = jax.nn.sigmoid(act)
    a[e] = (dh * up * sig * (1.0 + act * (1.0 - sig))).astype(BF16)
    b[e] = (dh * (act * sig)).astype(BF16)


def row_grads(e, cols, turned, w1t, w1, w3, a, b, dxr):
    if turned is None or e < turned:
        dx = jnp.dot(a[e], w1t[e, :, cols], preferred_element_type=F32)
    else:
        dx = lax.dot_general(a[e], w1[e, cols, :], TRANS_B, preferred_element_type=F32)
    if turned is None:
        dx = dx + jnp.dot(b[e], w3[e, :, cols], preferred_element_type=F32)
    else:
        dx = dx + lax.dot_general(b[e], w3[e, cols, :], TRANS_B, preferred_element_type=F32)
    dx = dx.astype(BF16)
    for h in range(2):
        dxr[e * HALF_ROWS : (e + 1) * HALF_ROWS, h * (D // 2) : h * (D // 2) + dx.shape[1]] = dx[h * HALF_ROWS : (h + 1) * HALF_ROWS]


def return_sums(ids, core, x, y, scatter, turned, w1t, w1, w3, a, b, dxr, sums, inbox, send, recv, ssem, outs, between):
    def exchange(n, yy, xx):
        theirs = 4 * yy + 2 * xx + (1 - core)
        cols = pl.ds(*CHUNKS[n])
        src = sums.at[pl.ds(pl.multiple_of(theirs * TOK, TOK), TOK), cols]
        return pltpu.make_async_remote_copy(src_ref=src, dst_ref=inbox.at[2 * yy + xx, :, cols], send_sem=send.at[0], recv_sem=recv.at[n], device_id={"expert": ids["partner"]}, device_id_type=MESH)

    def whole(ref, sem):
        return pltpu.make_async_remote_copy(src_ref=ref, dst_ref=ref, send_sem=send.at[0], recv_sem=sem, device_id={"expert": ids["partner"]}, device_id_type=MESH)

    def store(n, name, xx, yy, out, k):
        cols = pl.ds(*CHUNKS[n])
        return pltpu.make_async_copy(inbox.at[2 * yy + xx, :, cols], out.at[:, cols], ssem.at[k])

    blocks = (("me", x, y, outs[0], 0), ("x", 1 - x, y, outs[1], 1), ("y", x, 1 - y, outs[2], 2), ("diag", 1 - x, 1 - y, outs[3], 3))

    def collect(n):
        cols = slice(CHUNKS[n][0], sum(CHUNKS[n]))
        whole(inbox.at[:, :, cols], recv.at[n]).wait_recv()
        for name, xx, yy, out, k in blocks:
            inbox[2 * yy + xx, :, cols] = inbox[2 * yy + xx, :, cols] + sums[pl.ds(pl.multiple_of(ids[name] * TOK, TOK), TOK), cols]
            store(n, name, xx, yy, out, k).start()

    for n in range(len(CHUNKS)):
        cols = slice(CHUNKS[n][0], sum(CHUNKS[n]))
        for e in range(LOCAL):
            row_grads(e, cols, turned, w1t, w1, w3, a, b, dxr)
        for h in range(2):
            sums[h * 256 : (h + 1) * 256, cols] = jnp.dot(scatter[h, :, 0 : LOCAL * HALF_ROWS], dxr[0 : LOCAL * HALF_ROWS, h * (D // 2) : h * (D // 2) + CHUNKS[n][1]], preferred_element_type=F32)
        for k in range(4):
            exchange(n, k // 2, k % 2).start()
        if n == 2:
            collect(0)
        between(n)
    collect(1)
    collect(2)
    whole(inbox, recv.at[0]).wait_send()
    for name, xx, yy, out, k in blocks:
        pltpu.make_async_copy(inbox.at[2 * yy + xx], out, ssem.at[k]).wait()


class Weights:
    def __init__(self, hbm, vmem, sems):
        self.hbm, self.vmem, self.sems = hbm, vmem, sems

    def copy(self, k, e):
        return pltpu.make_async_copy(self.hbm[k].at[e], self.vmem[k].at[e], self.sems.at[k, e])

    def start(self, kinds, experts):
        for e in experts:
            for k in kinds:
                self.copy(k, e).start()

    def wait(self, kinds, e):
        for k in kinds:
            self.copy(k, e).wait()


def layer_two_kernel(*refs):
    routing_h, refs = refs[:6], refs[6:]
    (y_h, dy_h, x_h, w1_h, w3_h, w2_h,
     u_o, z_o, hid_o, da_o, db_o, xall_o, table_o, s_me, s_x, s_y, s_d) = refs[:17]
    routing, refs = refs[17:23], refs[23:]
    (tab, yall, dall, xall, w1, w3, w2, onehot, scatter, gate_col, w2t, u, z, a, b, hid, sums, inbox, w3t, table,
     lsem, wsem, osem, tsend, trecv, gsend, grecv, xsend, xrecv, ssem) = refs
    ids, core, x, y = place()
    greet(ids)
    small = [pltpu.make_async_copy(src, dst, lsem.at[3 + i]) for i, (src, dst) in enumerate(zip(routing_h, routing))]
    local = [pltpu.make_async_copy(src, block(dst, ids["me"]), lsem.at[i]) for i, (src, dst) in enumerate(((y_h, yall), (dy_h, dall), (x_h, xall)))]
    for c in small + local:
        c.start()
    for c in small:
        c.wait()
    fill_table(routing, ids["me"], tab.at[ids["me"]])
    local[0].wait()
    weights = Weights((w1_h, w3_h, w2_h), (w1, w3, w2), wsem)
    gt = Gather(ids, tab, tsend, trecv, 0)
    gy, gd, gx = [Gather(ids, ref, gsend.at[i], grecv.at[i], 2) for i, ref in enumerate((yall, dall, xall))]
    await_peers()
    gt.start(PRIM)
    gt.start(SEC)
    gy.start(PRIM)
    gt.start(PARTNER)
    weights.start((2,), range(LOCAL))
    for c in local[1:]:
        c.wait()
    weights.start((0, 1), range(LOCAL))

    def turn(first, last):
        for i in range(first, last):
            e = i % LOCAL
            if i < 2 * LOCAL:
                weights.wait(((2,), (0,))[i // LOCAL], e)
            (turn_wide, turn_tall, turn_tall)[i // LOCAL]((w2, w1, w3)[i // LOCAL], (w2t, w2, w3t)[i // LOCAL], e)

    turn(0, 1)
    gy.start(PARTNER)
    turn(1, 2)
    gy.start(SEC)
    turn(2, 3)
    gt.relay_prim(0)
    gy.relay_prim(0)
    turn(3, 5)
    gy.relay_prim(1)
    turn(5, 8)
    gd.start(PRIM)
    gt.relay_rest(0)
    turn(8, 9)
    gt.finish()
    join_table(tab, table)
    save_table = pltpu.make_async_copy(table, table_o, osem.at[6])
    save_table.start()
    build_onehot(table, 0, ids["me"], onehot, gate_col)
    gd.start(SEC)
    gd.start(PARTNER)
    gy.relay_rest(0)
    build_scatter(onehot, scatter)
    for e in range(LOCAL):
        weights.wait((1,), e)
    turn(9, 12)
    gy.relay_rest(1)
    turn(12, 13)
    gy.finish()
    gd.relay_prim(0)
    take_rows(onehot, yall, u)
    store_u = pltpu.make_async_copy(u, u_o, osem.at[0])
    store_u.start()

    def forward(first, last):
        lax.fori_loop(first, last, lambda e, carry: (forward_expert(e, u, w1, w3, a, b, hid), carry)[1], 0)

    gd.relay_prim(1)
    forward(0, 2)
    gx.start(PRIM)
    forward(2, 4)
    gx.start(SEC)
    gd.relay_rest(0)
    forward(4, LOCAL)
    gd.relay_rest(1)
    turn(13, 3 * LOCAL)
    gd.finish()
    gx.start(PARTNER)
    take_rows(onehot, dall, z, gate_col)
    store_z = pltpu.make_async_copy(z, z_o, osem.at[1])
    store_h = pltpu.make_async_copy(hid, hid_o, osem.at[2])
    store_z.start()
    store_h.start()
    gx.relay_prim(0)
    for e in range(LOCAL):
        hidden_grads(e, z, w2t, a, b)
    gx.relay_prim(1)
    store_a = pltpu.make_async_copy(a, da_o, osem.at[3])
    store_b = pltpu.make_async_copy(b, db_o, osem.at[4])
    store_a.start()
    store_b.start()
    store_x = pltpu.make_async_copy(xall, xall_o, osem.at[5])

    def between(n):
        if n == 1:
            gx.relay_rest(0)
            gx.relay_rest(1)
        if n == 2:
            gx.finish()
            store_x.start()

    gy.drain()
    return_sums(ids, core, x, y, scatter, None, w2, None, w3t, a, b, yall, sums, inbox, xsend, xrecv, ssem, (s_me, s_x, s_y, s_d), between)
    for g in (gt, gd, gx):
        g.drain()
    for c in (store_u, store_z, store_h, store_a, store_b, store_x, save_table):
        c.wait()


def layer_one_kernel(dy_h, r_me, r_x, r_y, r_d, table, xall_h, w1_h, w3_h, w2_h,
                     u_o, z_o, hid_o, da_o, db_o, dy1_o, s_me, s_x, s_y, s_d,
                     dall, xall, w1, w3, w2, onehot, scatter, gate_col, w2t, u, z, a, b, hid, sums, inbox,
                     lsem, wsem, osem, gsend, grecv, xsend, xrecv, ssem):
    ids, core, x, y = place()
    greet(ids)
    load_x = pltpu.make_async_copy(xall_h, xall, lsem.at[0])
    load_x.start()
    weights = Weights((w1_h, w3_h, w2_h), (w1, w3, w2), wsem)
    weights.start((0, 1), (0,))
    dy1 = (dy_h[...].astype(F32) + ((r_me[...] + r_x[...]) + (r_y[...] + r_d[...]))).astype(BF16)
    dall[pl.ds(pl.multiple_of(ids["me"] * TOK, TOK), TOK), :] = dy1
    dy1_o[...] = dy1
    await_peers()
    gd = Gather(ids, dall, gsend, grecv, 2)
    gd.start(PRIM)
    weights.start((2,), (0, 1))
    build_onehot(table, 16, ids["me"], onehot, gate_col)
    load_x.wait()
    weights.start((0, 1), (1,))
    weights.start((2,), (2, 3))
    weights.start((0, 1), (2, 3, 4))
    weights.start((2,), (4,))
    take_rows(onehot, xall, u)
    gd.start(SEC)
    gd.start(PARTNER)
    build_scatter(onehot, scatter)
    store_u = pltpu.make_async_copy(u, u_o, osem.at[0])
    store_u.start()

    def forward(first, last):
        def step(e, carry):
            weights.wait((0, 1), e)
            forward_expert(e, u, w1, w3, a, b, hid)
            return carry
        lax.fori_loop(first, last, step, 0)

    def turn(first, last):
        for i in range(first, last):
            e = i % LOCAL
            if i < LOCAL:
                weights.wait((2,), e)
                turn_wide(w2, w2t, e)
            else:
                turn_tall(w1, w2, e)

    forward(0, 1)
    turn(0, 2)
    gd.relay_prim(0)
    forward(1, 2)
    turn(2, 4)
    gd.relay_prim(1)
    forward(2, LOCAL)
    turn(4, 5)
    gd.relay_rest(0)
    turn(5, 7)
    gd.relay_rest(1)
    turn(7, LOCAL + TURNED)
    gd.finish()
    take_rows(onehot, dall, z, gate_col)
    store_z = pltpu.make_async_copy(z, z_o, osem.at[1])
    store_h = pltpu.make_async_copy(hid, hid_o, osem.at[2])
    store_z.start()
    store_h.start()
    for e in range(LOCAL):
        hidden_grads(e, z, w2t, a, b)
    store_a = pltpu.make_async_copy(a, da_o, osem.at[3])
    store_b = pltpu.make_async_copy(b, db_o, osem.at[4])
    store_a.start()
    store_b.start()
    return_sums(ids, core, x, y, scatter, TURNED, w2, w1, w3, a, b, xall, sums, inbox, xsend, xrecv, ssem, (s_me, s_x, s_y, s_d), lambda n: None)
    gd.drain()
    for c in (store_u, store_z, store_h, store_a, store_b):
        c.wait()


HBM_SPEC = pl.BlockSpec(memory_space=pltpu.HBM)
VMEM_SPEC = pl.BlockSpec(memory_space=pltpu.VMEM)


def compute_scratch():
    return [
        pltpu.VMEM((LOCAL, D, F), BF16), pltpu.VMEM((LOCAL, D, F), BF16), pltpu.VMEM((LOCAL, F, D), BF16),
        pltpu.VMEM((2, SLOTS, 256), BF16), pltpu.VMEM((2, 256, SLOTS), BF16), pltpu.VMEM((2, LOCAL * HALF_ROWS, 128), F32), pltpu.VMEM((LOCAL, D, F), BF16),
        pltpu.VMEM((LOCAL, ROWS, D), BF16), pltpu.VMEM((LOCAL, ROWS, D), BF16),
        pltpu.VMEM((LOCAL, ROWS, F), BF16), pltpu.VMEM((LOCAL, ROWS, F), BF16), pltpu.VMEM((LOCAL, ROWS, F), BF16),
        pltpu.VMEM((8 * TOK, D), F32), pltpu.VMEM((4, TOK, D), F32),
    ]


ROW_OUTS = [jax.ShapeDtypeStruct((LOCAL, ROWS, D), BF16)] * 2 + [jax.ShapeDtypeStruct((LOCAL, ROWS, F), BF16)] * 3
SUM_OUTS = [jax.ShapeDtypeStruct((TOK, D), F32)] * 4
DMA = pltpu.SemaphoreType.DMA


def layer_two(routing, y_mid, dy_out, x_tokens, w1, w3, w2):
    all_tok = pltpu.VMEM((8 * TOK, D), BF16)
    table_in = [pltpu.VMEM((8, TOK), t) for t in (jnp.int32, jnp.int32, F32)]
    return pl.pallas_call(
        layer_two_kernel, name="layer_two",
        out_shape=ROW_OUTS + [jax.ShapeDtypeStruct((8 * TOK, D), BF16), jax.ShapeDtypeStruct((32, 8 * TOK), F32)] + SUM_OUTS,
        in_specs=[HBM_SPEC] * 12, out_specs=[HBM_SPEC] * 11,
        scratch_shapes=table_in * 2 + [pltpu.VMEM((8, 32, 128), F32), all_tok, all_tok, all_tok] + compute_scratch() + [pltpu.VMEM((LOCAL, F, D), BF16), pltpu.VMEM((32, 8 * TOK), F32)]
        + [DMA((9,)), DMA((3, LOCAL)), DMA((7,)), DMA((1,)), DMA((4,)), DMA((3, 1)), DMA((3, 7)), DMA((1,)), DMA((len(CHUNKS),)), DMA((4,))],
        compiler_params=pltpu.CompilerParams(collective_id=0, has_side_effects=True, vmem_limit_bytes=63 * 2**20),
        cost_estimate=pl.CostEstimate(flops=16 * 10**9, bytes_accessed=36 * 2**20, transcendentals=0),
    )(*routing, y_mid, dy_out, x_tokens, w1, w3, w2)


def layer_one(dy_out, returned, table, xall, w1, w3, w2):
    all_tok = pltpu.VMEM((8 * TOK, D), BF16)
    return pl.pallas_call(
        layer_one_kernel, name="layer_one",
        out_shape=ROW_OUTS + [jax.ShapeDtypeStruct((TOK, D), BF16)] + SUM_OUTS,
        in_specs=[VMEM_SPEC] * 6 + [HBM_SPEC] * 4, out_specs=[HBM_SPEC] * 5 + [VMEM_SPEC] + [HBM_SPEC] * 4,
        scratch_shapes=[all_tok, all_tok] + compute_scratch()
        + [DMA((1,)), DMA((3, LOCAL)), DMA((5,)), DMA((1,)), DMA((7,)), DMA((1,)), DMA((len(CHUNKS),)), DMA((4,))],
        compiler_params=pltpu.CompilerParams(collective_id=1, has_side_effects=True, vmem_limit_bytes=50 * 2**20),
        cost_estimate=pl.CostEstimate(flops=16 * 10**9, bytes_accessed=36 * 2**20, transcendentals=0),
    )(dy_out, *returned, table, xall, w1, w3, w2)


PARTS = 4


def weight_grad_kernel(u_h, z_h, hid_h, da_h, db_h, dw1_h, dw3_h, dw2_h, u, z, hid, da, db, ring1, ring3, ring2, isem, osem):
    def load(e):
        return [pltpu.make_async_copy(src.at[e], dst.at[e], isem.at[k, e]) for k, (src, dst) in enumerate(((u_h, u), (da_h, da), (db_h, db), (hid_h, hid), (z_h, z)))]

    for e in range(LOCAL):
        for c in load(e):
            c.start()

    def store(e, p):
        rows, cols = D // PARTS, F // PARTS
        return [pltpu.make_async_copy(ring1.at[p], dw1_h.at[e, pl.ds(p * rows, rows)], osem.at[0, p]),
                pltpu.make_async_copy(ring3.at[p], dw3_h.at[e, pl.ds(p * rows, rows)], osem.at[1, p]),
                pltpu.make_async_copy(ring2.at[p], dw2_h.at[e, pl.ds(p * cols, cols)], osem.at[2, p])]

    def expert(e, carry):
        for c in load(e):
            c.wait()
        for p in range(PARTS):
            rows, cols = slice(p * (D // PARTS), (p + 1) * (D // PARTS)), slice(p * (F // PARTS), (p + 1) * (F // PARTS))
            out = store(e, p)

            @pl.when(e > 0)
            def _():
                for c in out:
                    c.wait()

            ring1[p] = lax.dot_general(u[e, :, rows], da[e], TRANS_A, preferred_element_type=F32)
            out[0].start()
            ring3[p] = lax.dot_general(u[e, :, rows], db[e], TRANS_A, preferred_element_type=F32)
            out[1].start()
            ring2[p] = lax.dot_general(hid[e, :, cols], z[e], TRANS_A, preferred_element_type=F32)
            out[2].start()
        return carry

    lax.fori_loop(0, LOCAL, expert, 0)
    for p in range(PARTS):
        for c in store(LOCAL - 1, p):
            c.wait()


def weight_grads(u, z, hid, da, db):
    wide, narrow = pltpu.VMEM((LOCAL, ROWS, D), BF16), pltpu.VMEM((LOCAL, ROWS, F), BF16)
    ring = pltpu.VMEM((PARTS, D // PARTS, F), F32)
    return pl.pallas_call(
        weight_grad_kernel, name="weight_grads",
        in_specs=[HBM_SPEC] * 5, out_specs=[HBM_SPEC] * 3,
        out_shape=[jax.ShapeDtypeStruct((LOCAL, D, F), F32)] * 2 + [jax.ShapeDtypeStruct((LOCAL, F, D), F32)],
        scratch_shapes=[wide, wide, narrow, narrow, narrow, ring, ring, pltpu.VMEM((PARTS, F // PARTS, D), F32), DMA((5, LOCAL)), DMA((3, PARTS))],
        compiler_params=pltpu.CompilerParams(vmem_limit_bytes=60 * 2**20),
        cost_estimate=pl.CostEstimate(flops=18 * 10**9, bytes_accessed=56 * 2**20, transcendentals=0),
    )(u, z, hid, da, db)


def exchange_sums(sums):
    swap = lambda mask: [(i, i ^ mask) for i in range(8)]
    return (sums[0],) + tuple(lax.ppermute(sums[k], "expert", swap(mask)) for k, mask in ((1, 2), (2, 4), (3, 6)))


def solution(mesh):
    tok_spec = P(("data", "expert"), None)
    weight_spec = P("expert", None, None)
    grad_spec = P(("data", "expert"), None, None)

    def local_step(x_tokens, y_mid, dy_out, experts_one, gates_one, slots_one, experts_two, gates_two, slots_two, w_gate_one, w_up_one, w_down_one, w_gate_two, w_up_two, w_down_two):
        routing = [r.T for r in (experts_two, slots_two, gates_two, experts_one, slots_one, gates_one)]
        *rows_two, xall, table, s0, s1, s2, s3 = layer_two(routing, y_mid, dy_out, x_tokens, w_gate_two, w_up_two, w_down_two)
        returned = exchange_sums((s0, s1, s2, s3))
        grads_two = weight_grads(*rows_two)
        *rows_one, dy_mid, s0, s1, s2, s3 = layer_one(dy_out, returned, table, xall, w_gate_one, w_up_one, w_down_one)
        r = exchange_sums((s0, s1, s2, s3))
        grads_one = weight_grads(*rows_one)
        dx_tokens = (dy_mid.astype(F32) + ((r[0] + r[1]) + (r[2] + r[3]))).astype(BF16)
        return (dx_tokens, *grads_one, *grads_two)

    return jax.shard_map(local_step, mesh=mesh, in_specs=(tok_spec,) * 9 + (weight_spec,) * 6, out_specs=(tok_spec,) + (grad_spec,) * 6, check_vma=False)
```

```python
import functools
import jax
import jax.numpy as jnp
from jax import lax
from jax.experimental import pallas as pl
from jax.experimental.pallas import tpu as pltpu
from jax.sharding import PartitionSpec as P

MESH = pl.DeviceIdType.MESH
F32 = jnp.float32
BF16 = jnp.bfloat16
CAP = 24
LOCAL = 5
D = 1536
F = 512
TOK = 64
HALF_ROWS = 4 * CAP
ROWS = 8 * CAP
STEP = 512
SLOTS = 512
TURNED = 5
CHUNKS = ((0, 768), (768, 512), (1280, 256))


def place():
    me = lax.axis_index("expert")
    core, x, y = me % 2, (me // 2) % 2, me // 4
    ident = lambda xx, yy, cc: 4 * yy + 2 * xx + cc
    ids = {
        "me": me,
        "partner": ident(x, y, 1 - core),
        "x": ident(1 - x, y, core),
        "y": ident(x, 1 - y, core),
        "diag": ident(1 - x, 1 - y, core),
        "prim": ident(x + (1 - core) * (1 - 2 * x), y + core * (1 - 2 * y), core),
        "sec": ident(x + core * (1 - 2 * x), y + (1 - core) * (1 - 2 * y), core),
        "p_prim": ident(x + core * (1 - 2 * x), y + (1 - core) * (1 - 2 * y), 1 - core),
        "p_sec": ident(x + (1 - core) * (1 - 2 * x), y + core * (1 - 2 * y), 1 - core),
        "p_diag": ident(1 - x, 1 - y, 1 - core),
    }
    return ids, core, x, y


def greet(ids):
    for peer in ("partner", "x", "y"):
        pl.semaphore_signal(pltpu.get_barrier_semaphore(), inc=1, device_id={"expert": ids[peer]}, device_id_type=MESH)


def await_peers():
    pl.semaphore_wait(pltpu.get_barrier_semaphore(), 3)


def block(ref, ident):
    return ref.at[pl.ds(pl.multiple_of(ident * TOK, TOK), TOK)]


class Gather:
    ROUTES = (("me", "partner"), ("me", "prim"), ("me", "sec"), ("prim", "sec"), ("prim", "partner"), ("sec", "partner"), ("diag", "partner"))
    ARRIVE = ("partner", "prim", "sec", "diag", "p_prim", "p_sec", "p_diag")

    def __init__(self, ids, ref, send, recv, pieces):
        self.ids, self.ref, self.send, self.recv, self.pieces = ids, ref, send, recv, pieces

    def part(self, ident, i):
        if self.pieces == 0:
            return self.ref.at[ident]
        size = TOK // self.pieces
        return self.ref.at[pl.ds(pl.multiple_of(ident * TOK + i * size, size), size)]

    def arrival(self, k, i):
        return self.recv.at[3 * i + k - 1] if 1 <= k <= 3 else self.recv.at[3 * max(self.pieces, 1)]

    def copy(self, k, i, what=None, where=None):
        what, where = what or self.ROUTES[k][0], where or self.ROUTES[k][1]
        part = self.part(self.ids[what], i)
        return pltpu.make_async_remote_copy(src_ref=part, dst_ref=part, send_sem=self.send.at[0], recv_sem=self.arrival(k, i), device_id={"expert": self.ids[where]}, device_id_type=MESH)

    def arrived(self, k, i):
        self.copy(k, i, self.ARRIVE[k], "partner").wait_recv()

    def every(self):
        return range(max(self.pieces, 1))

    def start(self, k):
        for i in self.every():
            self.copy(k, i).start()

    def relay_prim(self, i):
        self.arrived(1, i)
        self.copy(3, i).start()
        self.copy(4, i).start()

    def relay_rest(self, i):
        self.arrived(2, i)
        self.copy(5, i).start()
        self.arrived(3, i)
        self.copy(6, i).start()

    def blocks(self, count):
        part = self.ref.at[pl.ds(0, count * (TOK if self.pieces else 1))]
        return pltpu.make_async_remote_copy(src_ref=part, dst_ref=part, send_sem=self.send.at[0], recv_sem=self.recv.at[3 * max(self.pieces, 1)], device_id={"expert": self.ids["partner"]}, device_id_type=MESH)

    def finish(self):
        self.blocks(4).wait_recv()

    def drain(self):
        self.blocks(7).wait_send()


PARTNER, PRIM, SEC = 0, 1, 2


def fill_table(routing, me, out):
    out[...] = jnp.zeros((32, 128), F32)
    for layer in range(2):
        experts, slots, gates = (routing[3 * layer + k] for k in range(3))
        keys = jnp.where(slots[...] >= 0, experts[...] * HALF_ROWS + (me % 4) * CAP + slots[...], -1)
        out[16 * layer : 16 * layer + 8, 0:TOK] = keys.astype(F32)
        out[16 * layer + 8 : 16 * layer + 16, 0:TOK] = gates[...]


def join_table(tab, table):
    low = lax.broadcasted_iota(jnp.int32, (32, 128), 1) < TOK
    for p in range(4):
        table[:, p * 128 : (p + 1) * 128] = jnp.where(low, tab[2 * p], pltpu.roll(tab[2 * p + 1], TOK, 1))


def build_onehot(table, base, me, onehot, gate_col):
    for h in range(2):
        onehot[h, LOCAL * HALF_ROWS : SLOTS, :] = jnp.zeros((SLOTS - LOCAL * HALF_ROWS, 256), BF16)
        cols = slice(h * 256, (h + 1) * 256)
        keys = [table[base + j : base + j + 1, cols] for j in range(8)]
        gates = [table[base + 8 + j : base + 9 + j, cols] for j in range(8)]
        for e in range(LOCAL):
            row = (lax.broadcasted_iota(jnp.int32, (HALF_ROWS, 256), 0) + (e + me * LOCAL) * HALF_ROWS).astype(F32)
            gate = jnp.zeros((HALF_ROWS, 256), F32)
            hit = jnp.zeros((HALF_ROWS, 256), F32)
            for j in range(8):
                match = row == keys[j]
                gate = jnp.where(match, gates[j], gate)
                hit = jnp.where(match, 1.0, hit)
            onehot[h, e * HALF_ROWS : (e + 1) * HALF_ROWS, :] = hit.astype(BF16)
            gate_col[h, e * HALF_ROWS : (e + 1) * HALF_ROWS, :] = jnp.broadcast_to(jnp.sum(gate, axis=1, keepdims=True), (HALF_ROWS, 128))


def build_scatter(onehot, scatter):
    for h in range(2):
        scatter[h] = jnp.transpose(onehot[h])


def turn_tall(src, dst, e):
    for n in range(D // 128):
        dst[e, :, n * 128 : (n + 1) * 128] = jnp.transpose(src[e, n * 128 : (n + 1) * 128, :])


def turn_wide(src, dst, e):
    for n in range(D // 128):
        dst[e, n * 128 : (n + 1) * 128, :] = jnp.transpose(src[e, :, n * 128 : (n + 1) * 128])


def take_rows(onehot, tokens, rows, gate_col=None):
    for h in range(2):
        for n in range(D // STEP):
            cols = slice(n * STEP, (n + 1) * STEP)
            out = jnp.dot(onehot[h, 0 : LOCAL * HALF_ROWS], tokens[h * 256 : (h + 1) * 256, cols], preferred_element_type=F32)
            if gate_col is not None:
                out = out * gate_col[h, :, 0:1]
            out = out.astype(BF16)
            for e in range(LOCAL):
                rows[e, h * HALF_ROWS : (h + 1) * HALF_ROWS, cols] = out[e * HALF_ROWS : (e + 1) * HALF_ROWS]


def forward_expert(e, u, w1, w3, a, b, hid):
    act = jnp.dot(u[e], w1[e], preferred_element_type=F32).astype(BF16)
    up = jnp.dot(u[e], w3[e], preferred_element_type=F32).astype(BF16)
    a[e] = act
    b[e] = up
    wide = act.astype(F32)
    hid[e] = (wide * jax.nn.sigmoid(wide) * up.astype(F32)).astype(BF16)


TRANS_B = (((1,), (1,)), ((), ()))
TRANS_A = (((0,), (0,)), ((), ()))


def hidden_grads(e, z, w2, a, b):
    dh = jnp.dot(z[e], w2[e], preferred_element_type=F32)
    act = a[e].astype(F32)
    up = b[e].astype(F32)
    sig = jax.nn.sigmoid(act)
    a[e] = (dh * up * sig * (1.0 + act * (1.0 - sig))).astype(BF16)
    b[e] = (dh * (act * sig)).astype(BF16)


def row_grads(e, cols, turned, w1t, w1, w3, a, b, dxr):
    if turned is None or e < turned:
        dx = jnp.dot(a[e], w1t[e, :, cols], preferred_element_type=F32)
    else:
        dx = lax.dot_general(a[e], w1[e, cols, :], TRANS_B, preferred_element_type=F32)
    if turned is None:
        dx = dx + jnp.dot(b[e], w3[e, :, cols], preferred_element_type=F32)
    else:
        dx = dx + lax.dot_general(b[e], w3[e, cols, :], TRANS_B, preferred_element_type=F32)
    dx = dx.astype(BF16)
    for h in range(2):
        dxr[e * HALF_ROWS : (e + 1) * HALF_ROWS, h * (D // 2) : h * (D // 2) + dx.shape[1]] = dx[h * HALF_ROWS : (h + 1) * HALF_ROWS]


def return_sums(ids, core, x, y, scatter, turned, w1t, w1, w3, a, b, dxr, sums, inbox, send, recv, ssem, outs, between):
    def exchange(n, yy, xx):
        theirs = 4 * yy + 2 * xx + (1 - core)
        cols = pl.ds(*CHUNKS[n])
        src = sums.at[pl.ds(pl.multiple_of(theirs * TOK, TOK), TOK), cols]
        return pltpu.make_async_remote_copy(src_ref=src, dst_ref=inbox.at[2 * yy + xx, :, cols], send_sem=send.at[0], recv_sem=recv.at[n], device_id={"expert": ids["partner"]}, device_id_type=MESH)

    def whole(ref, sem):
        return pltpu.make_async_remote_copy(src_ref=ref, dst_ref=ref, send_sem=send.at[0], recv_sem=sem, device_id={"expert": ids["partner"]}, device_id_type=MESH)

    def store(n, name, xx, yy, out, k):
        cols = pl.ds(*CHUNKS[n])
        return pltpu.make_async_copy(inbox.at[2 * yy + xx, :, cols], out.at[:, cols], ssem.at[k])

    blocks = (("me", x, y, outs[0], 0), ("x", 1 - x, y, outs[1], 1), ("y", x, 1 - y, outs[2], 2), ("diag", 1 - x, 1 - y, outs[3], 3))

    def collect(n):
        cols = slice(CHUNKS[n][0], sum(CHUNKS[n]))
        whole(inbox.at[:, :, cols], recv.at[n]).wait_recv()
        for name, xx, yy, out, k in blocks:
            inbox[2 * yy + xx, :, cols] = inbox[2 * yy + xx, :, cols] + sums[pl.ds(pl.multiple_of(ids[name] * TOK, TOK), TOK), cols]
            store(n, name, xx, yy, out, k).start()

    for n in range(len(CHUNKS)):
        cols = slice(CHUNKS[n][0], sum(CHUNKS[n]))
        for e in range(LOCAL):
            row_grads(e, cols, turned, w1t, w1, w3, a, b, dxr)
        for h in range(2):
            sums[h * 256 : (h + 1) * 256, cols] = jnp.dot(scatter[h, :, 0 : LOCAL * HALF_ROWS], dxr[0 : LOCAL * HALF_ROWS, h * (D // 2) : h * (D // 2) + CHUNKS[n][1]], preferred_element_type=F32)
        for k in range(4):
            exchange(n, k // 2, k % 2).start()
        if n == 2:
            collect(0)
        between(n)
    collect(1)
    collect(2)
    whole(inbox, recv.at[0]).wait_send()
    for name, xx, yy, out, k in blocks:
        pltpu.make_async_copy(inbox.at[2 * yy + xx], out, ssem.at[k]).wait()


class Weights:
    def __init__(self, hbm, vmem, sems):
        self.hbm, self.vmem, self.sems = hbm, vmem, sems

    def copy(self, k, e):
        return pltpu.make_async_copy(self.hbm[k].at[e], self.vmem[k].at[e], self.sems.at[k, e])

    def start(self, kinds, experts):
        for e in experts:
            for k in kinds:
                self.copy(k, e).start()

    def wait(self, kinds, e):
        for k in kinds:
            self.copy(k, e).wait()


def layer_two_kernel(*refs):
    routing_h, refs = refs[:6], refs[6:]
    (y_h, dy_h, x_h, w1_h, w3_h, w2_h,
     u_o, z_o, hid_o, da_o, db_o, xall_o, table_o, s_me, s_x, s_y, s_d) = refs[:17]
    routing, refs = refs[17:23], refs[23:]
    (tab, yall, dall, xall, w1, w3, w2, onehot, scatter, gate_col, w2t, u, z, a, b, hid, sums, inbox, w3t, table,
     lsem, wsem, osem, tsend, trecv, gsend, grecv, xsend, xrecv, ssem) = refs
    ids, core, x, y = place()
    greet(ids)
    small = [pltpu.make_async_copy(src, dst, lsem.at[3 + i]) for i, (src, dst) in enumerate(zip(routing_h, routing))]
    local = [pltpu.make_async_copy(src, block(dst, ids["me"]), lsem.at[i]) for i, (src, dst) in enumerate(((y_h, yall), (dy_h, dall), (x_h, xall)))]
    for c in small + local:
        c.start()
    for c in small:
        c.wait()
    fill_table(routing, ids["me"], tab.at[ids["me"]])
    local[0].wait()
    weights = Weights((w1_h, w3_h, w2_h), (w1, w3, w2), wsem)
    gt = Gather(ids, tab, tsend, trecv, 0)
    gy, gd, gx = [Gather(ids, ref, gsend.at[i], grecv.at[i], 2) for i, ref in enumerate((yall, dall, xall))]
    await_peers()
    gt.start(PRIM)
    gt.start(SEC)
    gy.start(PRIM)
    gt.start(PARTNER)
    weights.start((2,), range(LOCAL))
    for c in local[1:]:
        c.wait()
    weights.start((0, 1), range(LOCAL))

    def turn(first, last):
        for i in range(first, last):
            e = i % LOCAL
            if i < 2 * LOCAL:
                weights.wait(((2,), (0,))[i // LOCAL], e)
            (turn_wide, turn_tall, turn_tall)[i // LOCAL]((w2, w1, w3)[i // LOCAL], (w2t, w2, w3t)[i // LOCAL], e)

    turn(0, 1)
    gy.start(PARTNER)
    turn(1, 2)
    gy.start(SEC)
    turn(2, 3)
    gt.relay_prim(0)
    gy.relay_prim(0)
    turn(3, 5)
    gy.relay_prim(1)
    turn(5, 8)
    gd.start(PRIM)
    gt.relay_rest(0)
    turn(8, 9)
    gt.finish()
    join_table(tab, table)
    save_table = pltpu.make_async_copy(table, table_o, osem.at[6])
    save_table.start()
    build_onehot(table, 0, ids["me"], onehot, gate_col)
    gd.start(SEC)
    gd.start(PARTNER)
    gy.relay_rest(0)
    build_scatter(onehot, scatter)
    for e in range(LOCAL):
        weights.wait((1,), e)
    turn(9, 12)
    gy.relay_rest(1)
    turn(12, 13)
    gy.finish()
    gd.relay_prim(0)
    take_rows(onehot, yall, u)
    store_u = pltpu.make_async_copy(u, u_o, osem.at[0])
    store_u.start()

    def forward(first, last):
        lax.fori_loop(first, last, lambda e, carry: (forward_expert(e, u, w1, w3, a, b, hid), carry)[1], 0)

    gd.relay_prim(1)
    forward(0, 2)
    gx.start(PRIM)
    forward(2, 4)
    gx.start(SEC)
    gd.relay_rest(0)
    forward(4, LOCAL)
    gd.relay_rest(1)
    turn(13, 3 * LOCAL)
    gd.finish()
    gx.start(PARTNER)
    take_rows(onehot, dall, z, gate_col)
    store_z = pltpu.make_async_copy(z, z_o, osem.at[1])
    store_h = pltpu.make_async_copy(hid, hid_o, osem.at[2])
    store_z.start()
    store_h.start()
    gx.relay_prim(0)
    for e in range(LOCAL):
        hidden_grads(e, z, w2t, a, b)
    gx.relay_prim(1)
    store_a = pltpu.make_async_copy(a, da_o, osem.at[3])
    store_b = pltpu.make_async_copy(b, db_o, osem.at[4])
    store_a.start()
    store_b.start()
    store_x = pltpu.make_async_copy(xall, xall_o, osem.at[5])

    def between(n):
        if n == 1:
            gx.relay_rest(0)
            gx.relay_rest(1)
        if n == 2:
            gx.finish()
            store_x.start()

    gy.drain()
    return_sums(ids, core, x, y, scatter, None, w2, None, w3t, a, b, yall, sums, inbox, xsend, xrecv, ssem, (s_me, s_x, s_y, s_d), between)
    for g in (gt, gd, gx):
        g.drain()
    for c in (store_u, store_z, store_h, store_a, store_b, store_x, save_table):
        c.wait()


def layer_one_kernel(dy_h, r_me, r_x, r_y, r_d, table, xall_h, w1_h, w3_h, w2_h,
                     u_o, z_o, hid_o, da_o, db_o, dy1_o, s_me, s_x, s_y, s_d,
                     dall, xall, w1, w3, w2, onehot, scatter, gate_col, w2t, u, z, a, b, hid, sums, inbox,
                     lsem, wsem, osem, gsend, grecv, xsend, xrecv, ssem):
    ids, core, x, y = place()
    greet(ids)
    load_x = pltpu.make_async_copy(xall_h, xall, lsem.at[0])
    load_x.start()
    weights = Weights((w1_h, w3_h, w2_h), (w1, w3, w2), wsem)
    weights.start((0, 1), (0,))
    dy1 = (dy_h[...].astype(F32) + ((r_me[...] + r_x[...]) + (r_y[...] + r_d[...]))).astype(BF16)
    dall[pl.ds(pl.multiple_of(ids["me"] * TOK, TOK), TOK), :] = dy1
    dy1_o[...] = dy1
    await_peers()
    gd = Gather(ids, dall, gsend, grecv, 2)
    gd.start(PRIM)
    weights.start((2,), (0, 1))
    build_onehot(table, 16, ids["me"], onehot, gate_col)
    load_x.wait()
    weights.start((0, 1), (1,))
    weights.start((2,), (2, 3))
    weights.start((0, 1), (2, 3, 4))
    weights.start((2,), (4,))
    take_rows(onehot, xall, u)
    gd.start(SEC)
    gd.start(PARTNER)
    build_scatter(onehot, scatter)
    store_u = pltpu.make_async_copy(u, u_o, osem.at[0])
    store_u.start()

    def forward(first, last):
        def step(e, carry):
            weights.wait((0, 1), e)
            forward_expert(e, u, w1, w3, a, b, hid)
            return carry
        lax.fori_loop(first, last, step, 0)

    def turn(first, last):
        for i in range(first, last):
            e = i % LOCAL
            if i < LOCAL:
                weights.wait((2,), e)
                turn_wide(w2, w2t, e)
            else:
                turn_tall(w1, w2, e)

    forward(0, 1)
    turn(0, 2)
    gd.relay_prim(0)
    forward(1, 2)
    turn(2, 4)
    gd.relay_prim(1)
    forward(2, LOCAL)
    turn(4, 5)
    gd.relay_rest(0)
    turn(5, 7)
    gd.relay_rest(1)
    turn(7, LOCAL + TURNED)
    gd.finish()
    take_rows(onehot, dall, z, gate_col)
    store_z = pltpu.make_async_copy(z, z_o, osem.at[1])
    store_h = pltpu.make_async_copy(hid, hid_o, osem.at[2])
    store_z.start()
    store_h.start()
    for e in range(LOCAL):
        hidden_grads(e, z, w2t, a, b)
    store_a = pltpu.make_async_copy(a, da_o, osem.at[3])
    store_b = pltpu.make_async_copy(b, db_o, osem.at[4])
    store_a.start()
    store_b.start()
    return_sums(ids, core, x, y, scatter, TURNED, w2, w1, w3, a, b, xall, sums, inbox, xsend, xrecv, ssem, (s_me, s_x, s_y, s_d), lambda n: None)
    gd.drain()
    for c in (store_u, store_z, store_h, store_a, store_b):
        c.wait()


HBM_SPEC = pl.BlockSpec(memory_space=pltpu.HBM)
VMEM_SPEC = pl.BlockSpec(memory_space=pltpu.VMEM)


def compute_scratch():
    return [
        pltpu.VMEM((LOCAL, D, F), BF16), pltpu.VMEM((LOCAL, D, F), BF16), pltpu.VMEM((LOCAL, F, D), BF16),
        pltpu.VMEM((2, SLOTS, 256), BF16), pltpu.VMEM((2, 256, SLOTS), BF16), pltpu.VMEM((2, LOCAL * HALF_ROWS, 128), F32), pltpu.VMEM((LOCAL, D, F), BF16),
        pltpu.VMEM((LOCAL, ROWS, D), BF16), pltpu.VMEM((LOCAL, ROWS, D), BF16),
        pltpu.VMEM((LOCAL, ROWS, F), BF16), pltpu.VMEM((LOCAL, ROWS, F), BF16), pltpu.VMEM((LOCAL, ROWS, F), BF16),
        pltpu.VMEM((8 * TOK, D), F32), pltpu.VMEM((4, TOK, D), F32),
    ]


ROW_OUTS = [jax.ShapeDtypeStruct((LOCAL, ROWS, D), BF16)] * 2 + [jax.ShapeDtypeStruct((LOCAL, ROWS, F), BF16)] * 3
SUM_OUTS = [jax.ShapeDtypeStruct((TOK, D), F32)] * 4
DMA = pltpu.SemaphoreType.DMA


def layer_two(routing, y_mid, dy_out, x_tokens, w1, w3, w2):
    all_tok = pltpu.VMEM((8 * TOK, D), BF16)
    table_in = [pltpu.VMEM((8, TOK), t) for t in (jnp.int32, jnp.int32, F32)]
    return pl.pallas_call(
        layer_two_kernel, name="layer_two",
        out_shape=ROW_OUTS + [jax.ShapeDtypeStruct((8 * TOK, D), BF16), jax.ShapeDtypeStruct((32, 8 * TOK), F32)] + SUM_OUTS,
        in_specs=[HBM_SPEC] * 12, out_specs=[HBM_SPEC] * 11,
        scratch_shapes=table_in * 2 + [pltpu.VMEM((8, 32, 128), F32), all_tok, all_tok, all_tok] + compute_scratch() + [pltpu.VMEM((LOCAL, F, D), BF16), pltpu.VMEM((32, 8 * TOK), F32)]
        + [DMA((9,)), DMA((3, LOCAL)), DMA((7,)), DMA((1,)), DMA((4,)), DMA((3, 1)), DMA((3, 7)), DMA((1,)), DMA((len(CHUNKS),)), DMA((4,))],
        compiler_params=pltpu.CompilerParams(collective_id=0, has_side_effects=True, vmem_limit_bytes=63 * 2**20),
        cost_estimate=pl.CostEstimate(flops=16 * 10**9, bytes_accessed=36 * 2**20, transcendentals=0),
    )(*routing, y_mid, dy_out, x_tokens, w1, w3, w2)


def layer_one(dy_out, returned, table, xall, w1, w3, w2):
    all_tok = pltpu.VMEM((8 * TOK, D), BF16)
    return pl.pallas_call(
        layer_one_kernel, name="layer_one",
        out_shape=ROW_OUTS + [jax.ShapeDtypeStruct((TOK, D), BF16)] + SUM_OUTS,
        in_specs=[VMEM_SPEC] * 6 + [HBM_SPEC] * 4, out_specs=[HBM_SPEC] * 5 + [VMEM_SPEC] + [HBM_SPEC] * 4,
        scratch_shapes=[all_tok, all_tok] + compute_scratch()
        + [DMA((1,)), DMA((3, LOCAL)), DMA((5,)), DMA((1,)), DMA((7,)), DMA((1,)), DMA((len(CHUNKS),)), DMA((4,))],
        compiler_params=pltpu.CompilerParams(collective_id=1, has_side_effects=True, vmem_limit_bytes=50 * 2**20),
        cost_estimate=pl.CostEstimate(flops=16 * 10**9, bytes_accessed=36 * 2**20, transcendentals=0),
    )(dy_out, *returned, table, xall, w1, w3, w2)


PARTS = 4


def weight_grad_kernel(u_h, z_h, hid_h, da_h, db_h, dw1_h, dw3_h, dw2_h, u, z, hid, da, db, ring1, ring3, ring2, isem, osem):
    def load(e):
        return [pltpu.make_async_copy(src.at[e], dst.at[e], isem.at[k, e]) for k, (src, dst) in enumerate(((u_h, u), (da_h, da), (db_h, db), (hid_h, hid), (z_h, z)))]

    for e in range(LOCAL):
        for c in load(e):
            c.start()

    def store(e, p):
        rows, cols = D // PARTS, F // PARTS
        return [pltpu.make_async_copy(ring1.at[p], dw1_h.at[e, pl.ds(p * rows, rows)], osem.at[0, p]),
                pltpu.make_async_copy(ring3.at[p], dw3_h.at[e, pl.ds(p * rows, rows)], osem.at[1, p]),
                pltpu.make_async_copy(ring2.at[p], dw2_h.at[e, pl.ds(p * cols, cols)], osem.at[2, p])]

    def expert(e, carry):
        for c in load(e):
            c.wait()
        for p in range(PARTS):
            rows, cols = slice(p * (D // PARTS), (p + 1) * (D // PARTS)), slice(p * (F // PARTS), (p + 1) * (F // PARTS))
            out = store(e, p)

            @pl.when(e > 0)
            def _():
                for c in out:
                    c.wait()

            ring1[p] = lax.dot_general(u[e, :, rows], da[e], TRANS_A, preferred_element_type=F32)
            out[0].start()
            ring3[p] = lax.dot_general(u[e, :, rows], db[e], TRANS_A, preferred_element_type=F32)
            out[1].start()
            ring2[p] = lax.dot_general(hid[e, :, cols], z[e], TRANS_A, preferred_element_type=F32)
            out[2].start()
        return carry

    lax.fori_loop(0, LOCAL, expert, 0)
    for p in range(PARTS):
        for c in store(LOCAL - 1, p):
            c.wait()


def weight_grads(u, z, hid, da, db):
    wide, narrow = pltpu.VMEM((LOCAL, ROWS, D), BF16), pltpu.VMEM((LOCAL, ROWS, F), BF16)
    ring = pltpu.VMEM((PARTS, D // PARTS, F), F32)
    return pl.pallas_call(
        weight_grad_kernel, name="weight_grads",
        in_specs=[HBM_SPEC] * 5, out_specs=[HBM_SPEC] * 3,
        out_shape=[jax.ShapeDtypeStruct((LOCAL, D, F), F32)] * 2 + [jax.ShapeDtypeStruct((LOCAL, F, D), F32)],
        scratch_shapes=[wide, wide, narrow, narrow, narrow, ring, ring, pltpu.VMEM((PARTS, F // PARTS, D), F32), DMA((5, LOCAL)), DMA((3, PARTS))],
        compiler_params=pltpu.CompilerParams(vmem_limit_bytes=60 * 2**20),
        cost_estimate=pl.CostEstimate(flops=18 * 10**9, bytes_accessed=56 * 2**20, transcendentals=0),
    )(u, z, hid, da, db)


def exchange_sums(sums):
    swap = lambda mask: [(i, i ^ mask) for i in range(8)]
    return (sums[0],) + tuple(lax.ppermute(sums[k], "expert", swap(mask)) for k, mask in ((3, 6), (1, 2), (2, 4)))


def solution(mesh):
    tok_spec = P(("data", "expert"), None)
    weight_spec = P("expert", None, None)
    grad_spec = P(("data", "expert"), None, None)

    def local_step(x_tokens, y_mid, dy_out, experts_one, gates_one, slots_one, experts_two, gates_two, slots_two, w_gate_one, w_up_one, w_down_one, w_gate_two, w_up_two, w_down_two):
        routing = [r.T for r in (experts_two, slots_two, gates_two, experts_one, slots_one, gates_one)]
        *rows_two, xall, table, s0, s1, s2, s3 = layer_two(routing, y_mid, dy_out, x_tokens, w_gate_two, w_up_two, w_down_two)
        returned = exchange_sums((s0, s1, s2, s3))
        grads_two = weight_grads(*rows_two)
        *rows_one, dy_mid, s0, s1, s2, s3 = layer_one(dy_out, returned, table, xall, w_gate_one, w_up_one, w_down_one)
        r = exchange_sums((s0, s1, s2, s3))
        grads_one = weight_grads(*rows_one)
        dx_tokens = (dy_mid.astype(F32) + ((r[0] + r[1]) + (r[2] + r[3]))).astype(BF16)
        return (dx_tokens, *grads_one, *grads_two)

    return jax.shard_map(local_step, mesh=mesh, in_specs=(tok_spec,) * 9 + (weight_spec,) * 6, out_specs=(tok_spec,) + (grad_spec,) * 6, check_vma=False)
```
